32 devices in a mesh: row: 8 (over z, x), col: 2 (over core), dp: 2 (over y).
Axes of the slice: x: 2, y: 2, z: 4, core: 2. Of those that a mesh axis runs over, the one named last changes fastest.
Arguments:
- pixels: bfloat16 [2, 3, 256, 256], P('dp', None, 'row', 'col'), may hold values from -6 to 6
- cotangent: bfloat16 [2, 64, 64, 1024], P('dp', 'row', 'col'), may hold values from -6 to 6
- embed_weight: bfloat16 [48, 1024], replicated, may hold values from -0.875 to 0.875
- embed_bias: float32 [1024], replicated, may hold values from -4 to 4
- layer_norm_gain: float32 [1024], replicated, may hold values from 0.5 to 1.5
- qkv_weight: bfloat16 [1024, 2304], P('row', ('col', 'dp')), may hold values from -0.1875 to 0.1875
- out_weight: bfloat16 [768, 1024], P('row', ('col', 'dp')), may hold values from -0.21875 to 0.21875
- bias_table: float32 [12, 225], replicated, may hold values from -4 to 404
- rel_index: int32 [64, 64], replicated, may hold values from 0 to 224
- shifts: int32 [2, 2], P('dp'), may hold values from 1 to 7
Outputs:
- out_weight_grad: float32 [768, 1024], P('row', ('col', 'dp'))
- embed_weight_grad: float32 [48, 1024], replicated
- embed_bias_grad: float32 [1024], replicated
- norm_gain_grad: float32 [1024], replicated
- bias_table_grad: float32 [12, 225], replicated
The draws below stay inside these ranges and needn't reach their ends.
Inputs may be any that keep to these rules, and one draw needn't show every extreme that they name: `rel_index`: each entry names one of the 225 columns of bias_table.
All inputs are finite; a program needn't handle non-finite values.
Results may differ from the reference program's by a relative error of at most 0.023.
Values may be sent and summed in bfloat16 or wider, within the bound.
A program may use at most 64 MiB of HBM per device.

```python
import jax
import jax.numpy as jnp
from jax import lax

D = 1024
HEADS = 12
WIN = 8
PATCH = 4
CHAN = 3
HD = 768
TABLE = 225
KDIM = 48
BATCH = 2
GRID_ROWS = 64
GRID_COLS = 64
PIX_ROWS = 256
PIX_COLS = 256


def draw_bias_table(key, part):
    key_base = jax.random.fold_in(key, 11)
    base_draw = jax.random.normal(key_base, (HEADS, TABLE), jnp.float32)
    return jnp.clip(base_draw, -4.0, 4.0)


def with_ends(entries, own_key, smallest, top_value):
    place = [jax.random.randint(jax.random.fold_in(own_key, axis), (), 0, length) for axis, length in enumerate(entries.shape)]
    longest = entries.shape.index(max(entries.shape))
    next_to = place[:longest] + [(place[longest] + 1) % entries.shape[longest]] + place[longest + 1:]
    return entries.at[tuple(place)].set(smallest).at[tuple(next_to)].set(top_value)


def block_levels(key, extent, shards, least, largest):
    factor_of = 1.0
    for dim, shards_of in shards:
        draws = jax.random.uniform(jax.random.fold_in(jax.random.fold_in(key, 6), dim), (shards_of,), jnp.float32, least / len(shards), largest / len(shards))
        factor_of = factor_of * jnp.repeat(jnp.exp(draws), extent[dim] // shards_of).reshape((-1,) + (1,) * (len(extent) - 1 - dim))
    return factor_of


def gaussian(own_key, dims, spread, most, pieces=(), kind=jnp.bfloat16):
    entries = spread * jax.random.normal(own_key, dims, jnp.float32)
    if pieces:
        entries = entries * block_levels(own_key, dims, pieces, -0.22, 0.18)
    return jnp.clip(entries, -most, most).astype(kind)


def setup_inputs(seed: int = 0) -> dict:
    splits = jax.random.split(jax.random.key(seed), 11)
    return {
        "pixels": gaussian(splits[0], (BATCH, CHAN, PIX_ROWS, PIX_COLS), 1.0, 6.0, ((0, 2), (2, 8), (3, 2))),
        "cotangent": gaussian(splits[1], (BATCH, GRID_ROWS, GRID_COLS, D), 1.0, 6.0, ((0, 2), (1, 8), (2, 2))),
        "embed_weight": gaussian(splits[2], (KDIM, D), KDIM ** -0.5, 0.875),
        "embed_bias": gaussian(splits[3], (D,), 1.0, 4.0, (), jnp.float32),
        "layer_norm_gain": jnp.clip(1.0 + 0.1 * jax.random.normal(splits[4], (D,), jnp.float32), 0.5, 1.5),
        "qkv_weight": gaussian(splits[5], (D, 3 * HD), D ** -0.5, 0.1875, ((0, 8), (1, 4))),
        "out_weight": gaussian(splits[6], (HD, D), HD ** -0.5, 0.21875, ((0, 8), (1, 4))),
        "bias_table": draw_bias_table(jax.random.fold_in(splits[10], 71), 0),
        "rel_index": with_ends(jax.random.randint(splits[8], (WIN * WIN, WIN * WIN), 0, TABLE), jax.random.fold_in(splits[8], 1), 0, TABLE - 1).astype(jnp.int32),
        "shifts": with_ends(jax.random.randint(splits[9], (BATCH, 2), 1, WIN), jax.random.fold_in(splits[9], 1), 1, WIN - 1).astype(jnp.int32),
    }


norm_epsilon = 1e-05

def make_patches(pixel_block):
    images, channels, pixel_rows, pixel_cols = pixel_block.shape
    grid_rows = pixel_rows // PATCH
    grid_cols = pixel_cols // PATCH
    shaped = pixel_block.reshape(images, channels, grid_rows, PATCH, grid_cols, PATCH)
    return shaped.transpose(0, 2, 4, 1, 3, 5).reshape(images, grid_rows, grid_cols, channels * PATCH * PATCH)

def window_split(block):
    rows_all, cols_all, features = block.shape
    shaped = block.reshape(rows_all // WIN, WIN, cols_all // WIN, WIN, features)
    return shaped.transpose(0, 2, 1, 3, 4).reshape(-1, WIN * WIN, features)

def window_join(windows, rows_all, cols_all):
    features = windows.shape[-1]
    shaped = windows.reshape(rows_all // WIN, cols_all // WIN, WIN, WIN, features)
    return shaped.transpose(0, 2, 1, 3, 4).reshape(rows_all, cols_all, features)

def window_grads(cell_windows, cot_windows, labels, layer_norm_gain, qkv_weight, out_weight, bias_full):
    window_count, cell_count, features = cell_windows.shape
    head_count = bias_full.shape[0]
    inner_width = out_weight.shape[0]
    head_size = inner_width // head_count
    score_scale = head_size ** (-0.5)
    flat_rows = cell_windows.reshape(-1, features).astype(jnp.float32)
    average = lax.optimization_barrier(jnp.mean(flat_rows, axis=-1, keepdims=True))
    centered_input = flat_rows - average
    inverse_deviation = lax.rsqrt(lax.optimization_barrier(jnp.mean(centered_input * centered_input, axis=-1, keepdims=True)) + norm_epsilon)
    standardized_rows = centered_input * inverse_deviation
    normalized_rows = (standardized_rows * layer_norm_gain).astype(jnp.bfloat16)
    projected = jnp.dot(normalized_rows, qkv_weight, preferred_element_type=jnp.float32).astype(jnp.bfloat16)
    head_shape = (window_count, cell_count, head_count, head_size)
    query_rows = projected[:, :inner_width].reshape(head_shape).astype(jnp.float32)
    key_vectors = projected[:, inner_width:2 * inner_width].reshape(head_shape).astype(jnp.float32)
    value_rows = projected[:, 2 * inner_width:].reshape(head_shape).astype(jnp.float32)
    scores = jnp.einsum('wmhd,wnhd->whmn', query_rows, key_vectors) * score_scale + bias_full[None]
    same_region = labels[:, None, :, None] == labels[:, None, None, :]
    scores = jnp.where(same_region, scores, -1e+30)
    row_peak = lax.optimization_barrier(jnp.max(scores, axis=-1, keepdims=True))
    exp_scores = jnp.exp(scores - row_peak)
    attention_weights = exp_scores / lax.optimization_barrier(jnp.sum(exp_scores, axis=-1, keepdims=True))
    reduced_probability = attention_weights.astype(jnp.bfloat16)
    attended = jnp.einsum('whmn,wnhd->wmhd', reduced_probability.astype(jnp.float32), value_rows).astype(jnp.bfloat16)
    cot_rows = cot_windows.reshape(-1, features)
    d_attended = jnp.dot(cot_rows, out_weight.T, preferred_element_type=jnp.float32).astype(jnp.bfloat16)
    d_heads = d_attended.reshape(head_shape).astype(jnp.float32)
    d_prob = jnp.einsum('wmhd,wnhd->whmn', d_heads, value_rows)
    d_values = jnp.einsum('whmn,wmhd->wnhd', reduced_probability.astype(jnp.float32), d_heads).astype(jnp.bfloat16)
    d_scores = attention_weights * (d_prob - lax.optimization_barrier(jnp.sum(attention_weights * d_prob, axis=-1, keepdims=True)))
    table_part = lax.optimization_barrier(jnp.sum(d_scores, axis=0))
    d_low = d_scores.astype(jnp.bfloat16).astype(jnp.float32)
    d_queries = (jnp.einsum('whmn,wnhd->wmhd', d_low, key_vectors) * score_scale).astype(jnp.bfloat16)
    d_keys = (jnp.einsum('whmn,wmhd->wnhd', d_low, query_rows) * score_scale).astype(jnp.bfloat16)
    total_row_count = flat_rows.shape[0]
    d_projected = jnp.concatenate([d_queries.reshape(total_row_count, inner_width), d_keys.reshape(total_row_count, inner_width), d_values.reshape(total_row_count, inner_width)], axis=1)
    normalized_gradient = jnp.dot(d_projected, qkv_weight.T, preferred_element_type=jnp.float32)
    gain_contribution = lax.optimization_barrier(jnp.sum(normalized_gradient * standardized_rows, axis=0))
    scaled_rows = normalized_gradient * layer_norm_gain
    branch_gradient = inverse_deviation * (scaled_rows - lax.optimization_barrier(jnp.mean(scaled_rows, axis=-1, keepdims=True)) - standardized_rows * lax.optimization_barrier(jnp.mean(scaled_rows * standardized_rows, axis=-1, keepdims=True)))
    attended_rows = attended.reshape(total_row_count, inner_width)
    return (branch_gradient.astype(jnp.bfloat16), attended_rows, gain_contribution, table_part)

def reference(pixels, cotangent, embed_weight, embed_bias, layer_norm_gain, qkv_weight, out_weight, bias_table, rel_index, shifts):
    images, grid_rows, grid_cols, features = cotangent.shape
    head_count = bias_table.shape[0]
    table_size = bias_table.shape[1]
    inner_width = out_weight.shape[0]
    patch_width = embed_weight.shape[0]
    selector = (rel_index.reshape(-1)[:, None] == jnp.arange(table_size, dtype=jnp.int32)[None, :]).astype(jnp.float32)
    bias_full = jnp.dot(selector, bias_table.T, precision=lax.Precision.HIGHEST).T.reshape(head_count, WIN * WIN, WIN * WIN)
    patches_all = make_patches(pixels)
    band_count = grid_rows // WIN

    def per_image(carry, inputs):
        out_grad, embed_grad, bias_grad, gain_grad, table_grad = carry
        patches, cot_image, shift_pair = inputs
        tokens = (jnp.dot(patches, embed_weight, preferred_element_type=jnp.float32) + embed_bias).astype(jnp.bfloat16)
        shifted = jnp.roll(jnp.roll(tokens, -shift_pair[0], axis=0), -shift_pair[1], axis=1)
        shifted_cot = jnp.roll(jnp.roll(cot_image, -shift_pair[0], axis=0), -shift_pair[1], axis=1)
        band_tokens = shifted.reshape(band_count, WIN, grid_cols, features)
        band_cots = shifted_cot.reshape(band_count, WIN, grid_cols, features)

        def per_band(inner, band_inputs):
            band_out, band_gain, band_table = inner
            band_x, band_c, band_index = band_inputs
            row_ids = band_index * WIN + jnp.arange(WIN, dtype=jnp.int32)
            col_ids = jnp.arange(grid_cols, dtype=jnp.int32)
            row_part = (row_ids[:, None] >= grid_rows - shift_pair[0]).astype(jnp.int32)
            col_part = (col_ids[None, :] >= grid_cols - shift_pair[1]).astype(jnp.int32)
            region = 2 * row_part + col_part
            labels = window_split(region[:, :, None])[:, :, 0]
            cell_windows = window_split(band_x)
            cot_windows = window_split(band_c)
            branch_gradient, attended_rows, gain_contribution, table_part = window_grads(cell_windows, cot_windows, labels, layer_norm_gain, qkv_weight, out_weight, bias_full)
            band_out = band_out + lax.dot_general(attended_rows, cot_windows.reshape(-1, features), (((0,), (0,)), ((), ())), preferred_element_type=jnp.float32)
            joined = window_join(branch_gradient.reshape(-1, WIN * WIN, features), WIN, grid_cols)
            return ((band_out, band_gain + gain_contribution, band_table + table_part), joined)
        band_ids = jnp.arange(band_count, dtype=jnp.int32)
        (out_grad, gain_grad, table_grad), d_bands = lax.scan(per_band, (out_grad, gain_grad, table_grad), (band_tokens, band_cots, band_ids))
        branch_gradient = d_bands.reshape(grid_rows, grid_cols, features)
        d_back = jnp.roll(jnp.roll(branch_gradient, shift_pair[0], axis=0), shift_pair[1], axis=1)
        patch_rows = patches.reshape(-1, patch_width)
        cot_rows = cot_image.reshape(-1, features)
        back_rows = d_back.reshape(-1, features)
        contract = (((0,), (0,)), ((), ()))
        embed_grad = embed_grad + lax.dot_general(patch_rows, cot_rows, contract, preferred_element_type=jnp.float32) + lax.dot_general(patch_rows, back_rows, contract, preferred_element_type=jnp.float32)
        bias_grad = bias_grad + lax.optimization_barrier(jnp.sum(cot_rows, axis=0, dtype=jnp.float32)) + lax.optimization_barrier(jnp.sum(back_rows, axis=0, dtype=jnp.float32))
        return ((out_grad, embed_grad, bias_grad, gain_grad, table_grad), None)
    initial = (jnp.zeros((inner_width, features), jnp.float32), jnp.zeros((patch_width, features), jnp.float32), jnp.zeros((features,), jnp.float32), jnp.zeros((features,), jnp.float32), jnp.zeros((head_count, WIN * WIN, WIN * WIN), jnp.float32))
    totals, unused = lax.scan(per_image, initial, (patches_all, cotangent, shifts))
    out_grad, embed_grad, bias_grad, gain_grad, table_grad = totals
    table_result = jnp.dot(table_grad.reshape(head_count, -1), selector, precision=lax.Precision.HIGHEST)
    return (out_grad, embed_grad, bias_grad, gain_grad, table_result)
```

```python
import functools

import jax
import jax.numpy as jnp
from jax import lax
from jax.experimental import pallas as pl
from jax.experimental.pallas import tpu as pltpu
from jax.sharding import PartitionSpec as P

WIN = 8
PATCH = 4


norm_epsilon = 1e-05


def from_behind(value, axis, steps):
    count = lax.axis_size(axis)
    pairs = [(source, (source + steps) % count) for source in range(count)]
    return lax.ppermute(value, axis, pairs)


def make_patches(pixel_block):
    images, channels, pixel_rows, pixel_cols = pixel_block.shape
    grid_rows = pixel_rows // PATCH
    grid_cols = pixel_cols // PATCH
    shaped = pixel_block.reshape(images, channels, grid_rows, PATCH, grid_cols, PATCH)
    return shaped.transpose(0, 2, 4, 1, 3, 5).reshape(
        images, grid_rows, grid_cols, channels * PATCH * PATCH
    )


def embed_cells(patches, embed_weight, embed_bias):
    return (jnp.dot(patches, embed_weight, preferred_element_type=jnp.float32) + embed_bias).astype(
        jnp.bfloat16
    )


def window_split(block):
    rows_all, cols_all, features = block.shape
    shaped = block.reshape(rows_all // WIN, WIN, cols_all // WIN, WIN, features)
    return shaped.transpose(0, 2, 1, 3, 4).reshape(-1, WIN * WIN, features)


def window_join(windows, rows_all, cols_all):
    features = windows.shape[-1]
    shaped = windows.reshape(rows_all // WIN, cols_all // WIN, WIN, WIN, features)
    return shaped.transpose(0, 2, 1, 3, 4).reshape(rows_all, cols_all, features)

def attend_forward(cell_windows, labels, layer_norm_gain, qkv_full, bias_full):
    window_count, cell_count, features = cell_windows.shape
    head_count = bias_full.shape[0]
    inner_width = qkv_full.shape[1] // 3
    head_size = inner_width // head_count
    score_scale = head_size ** (-0.5)
    flat_rows = cell_windows.reshape(-1, features).astype(jnp.float32)
    average = jnp.mean(flat_rows, axis=-1, keepdims=True)
    centered_input = flat_rows - average
    inverse_deviation = lax.rsqrt(
        jnp.mean(centered_input * centered_input, axis=-1, keepdims=True) + norm_epsilon
    )
    standardized_rows = centered_input * inverse_deviation
    normalized_rows = (standardized_rows * layer_norm_gain).astype(jnp.bfloat16)
    projected = jnp.dot(normalized_rows, qkv_full, preferred_element_type=jnp.float32).astype(
        jnp.bfloat16
    )
    head_shape = (window_count, cell_count, head_count, head_size)
    query_rows = projected[:, :inner_width].reshape(head_shape)
    key_vectors = projected[:, inner_width : 2 * inner_width].reshape(head_shape)
    value_rows = projected[:, 2 * inner_width :].reshape(head_shape)
    scores = (
        jnp.einsum("wmhd,wnhd->whmn", query_rows, key_vectors, preferred_element_type=jnp.float32)
        * score_scale
        + bias_full[None]
    )
    same_region = labels[:, None, :, None] == labels[:, None, None, :]
    scores = jnp.where(same_region, scores, -1e30)
    row_peak = jnp.max(scores, axis=-1, keepdims=True)
    exp_scores = jnp.exp(scores - row_peak)
    attention_weights = exp_scores / jnp.sum(exp_scores, axis=-1, keepdims=True)
    reduced_probability = attention_weights.astype(jnp.bfloat16)
    attended = jnp.einsum(
        "whmn,wnhd->wmhd", reduced_probability, value_rows, preferred_element_type=jnp.float32
    ).astype(jnp.bfloat16)
    stored_residuals = (
        standardized_rows,
        inverse_deviation,
        query_rows,
        key_vectors,
        value_rows,
        attention_weights,
        reduced_probability,
    )
    return (stored_residuals, attended.reshape(-1, inner_width))


def attend_backward(stored_residuals, d_attended, layer_norm_gain, qkv_full):
    (
        standardized_rows,
        inverse_deviation,
        query_rows,
        key_vectors,
        value_rows,
        attention_weights,
        reduced_probability,
    ) = stored_residuals
    head_shape = query_rows.shape
    score_scale = head_shape[3] ** (-0.5)
    total_row_count = standardized_rows.shape[0]
    inner_width = head_shape[2] * head_shape[3]
    d_heads = d_attended.reshape(head_shape)
    d_prob = jnp.einsum("wmhd,wnhd->whmn", d_heads, value_rows, preferred_element_type=jnp.float32)
    d_values = jnp.einsum(
        "whmn,wmhd->wnhd", reduced_probability, d_heads, preferred_element_type=jnp.float32
    ).astype(jnp.bfloat16)
    d_scores = attention_weights * (
        d_prob - jnp.sum(attention_weights * d_prob, axis=-1, keepdims=True)
    )
    table_part = jnp.sum(d_scores, axis=0)
    d_low = d_scores.astype(jnp.bfloat16)
    d_queries = (
        jnp.einsum("whmn,wnhd->wmhd", d_low, key_vectors, preferred_element_type=jnp.float32)
        * score_scale
    ).astype(jnp.bfloat16)
    d_keys = (
        jnp.einsum("whmn,wmhd->wnhd", d_low, query_rows, preferred_element_type=jnp.float32)
        * score_scale
    ).astype(jnp.bfloat16)
    d_projected = jnp.concatenate(
        [
            d_queries.reshape(total_row_count, inner_width),
            d_keys.reshape(total_row_count, inner_width),
            d_values.reshape(total_row_count, inner_width),
        ],
        axis=1,
    )
    normalized_gradient = lax.dot_general(
        d_projected, qkv_full, (((1,), (1,)), ((), ())), preferred_element_type=jnp.float32
    )
    gain_contribution = jnp.sum(normalized_gradient * standardized_rows, axis=0)
    scaled_rows = normalized_gradient * layer_norm_gain
    branch_gradient = inverse_deviation * (
        scaled_rows
        - jnp.mean(scaled_rows, axis=-1, keepdims=True)
        - standardized_rows * jnp.mean(scaled_rows * standardized_rows, axis=-1, keepdims=True)
    )
    return (branch_gradient.astype(jnp.bfloat16), gain_contribution, table_part)


MESH = pl.DeviceIdType.MESH
VMEM = pltpu.VMEM


def on_device(
    sizes,
    pixels,
    cotangent,
    embed_weight,
    embed_bias,
    layer_norm_gain,
    qkv_weight,
    out_weight,
    bias_table,
    rel_index,
    shifts,
):
    images, rows_dev, cols_dev, features = cotangent.shape
    rows, cols, dps = sizes
    head_count, table_size = bias_table.shape
    pix_block, cot_block = pixels[0], cotangent[0]
    row_shift, col_shift = shifts[0, 0], shifts[0, 1]
    qkv_full, out_full = [
        lax.all_gather(
            lax.all_gather(w, "row", axis=0, tiled=True), ("col", "dp"), axis=1, tiled=True
        )
        for w in (qkv_weight, out_weight)
    ]
    pix_r, cot_r = from_behind((pix_block, cot_block), "row", -1)
    pix_c, cot_c = from_behind((pix_block, cot_block[:, :WIN]), "col", -1)
    pix_x, cot_x = from_behind((pix_c, cot_c), "row", -1)
    wide_pix = jnp.concatenate(
        [
            jnp.concatenate([pix_block, pix_c[:, :, : WIN * PATCH]], axis=2),
            jnp.concatenate([pix_r, pix_x[:, :, : WIN * PATCH]], axis=2),
        ],
        axis=1,
    )
    wide_cot = jnp.concatenate(
        [
            jnp.concatenate([cot_block, cot_c], axis=1),
            jnp.concatenate([cot_r, cot_x], axis=1),
        ],
        axis=0,
    )
    wide_patches = make_patches(wide_pix[None])[0]
    patches = lax.dynamic_slice(
        wide_patches, (row_shift, col_shift, 0), (rows_dev, cols_dev, wide_patches.shape[2])
    )
    shifted_cot = lax.dynamic_slice(
        wide_cot, (row_shift, col_shift, 0), (rows_dev, cols_dev, features)
    )
    patch_rows = window_split(patches).reshape(-1, patches.shape[2])
    cot_flat = window_split(shifted_cot).reshape(-1, features)
    grid_rows, grid_cols = rows_dev * rows, cols_dev * cols
    row_ids = lax.axis_index("row") * rows_dev + jnp.arange(rows_dev, dtype=jnp.int32)
    col_ids = lax.axis_index("col") * cols_dev + jnp.arange(cols_dev, dtype=jnp.int32)
    row_part = (row_ids >= grid_rows - row_shift).astype(jnp.int32)
    col_part = (col_ids >= grid_cols - col_shift).astype(jnp.int32)
    region = 2 * row_part[:, None] + col_part[None, :]
    labels = window_split(region[:, :, None])[:, :, 0]
    selector = (
        rel_index.reshape(-1)[:, None] == jnp.arange(table_size, dtype=jnp.int32)[None, :]
    ).astype(jnp.float32)
    bias_full = jnp.dot(selector, bias_table.T, precision=lax.Precision.HIGHEST).T.reshape(
        head_count, WIN * WIN, WIN * WIN
    )
    cells = embed_cells(patch_rows, embed_weight, embed_bias)
    stored_residuals, attended = attend_forward(
        cells.reshape(-1, WIN * WIN, features), labels, layer_norm_gain, qkv_full, bias_full
    )
    d_attended = lax.dot_general(
        cot_flat, out_full, (((1,), (1,)), ((), ())), preferred_element_type=jnp.float32
    ).astype(jnp.bfloat16)
    d_rows, gain_contribution, table_part = attend_backward(
        stored_residuals, d_attended, layer_norm_gain, qkv_full
    )
    table_grad = jnp.dot(
        table_part.reshape(head_count, -1), selector, precision=lax.Precision.HIGHEST
    )
    contract = (((0,), (0,)), ((), ()))
    back_rows = jnp.concatenate([cot_flat, d_rows], axis=0)
    embed_grad = lax.dot_general(
        jnp.concatenate([patch_rows, patch_rows], axis=0),
        back_rows,
        contract,
        preferred_element_type=jnp.float32,
    )
    bias_grad = jnp.sum(back_rows, axis=0, dtype=jnp.float32)
    partial_rows = lax.psum_scatter(
        lax.dot_general(attended, cot_flat, contract, preferred_element_type=jnp.float32),
        "row",
        scatter_dimension=0,
        tiled=True,
    )
    out_weight_grad = lax.psum_scatter(
        partial_rows, ("col", "dp"), scatter_dimension=1, tiled=True
    )
    totals = lax.psum(
        (embed_grad, bias_grad, gain_contribution, table_grad), ("row", "col", "dp")
    )
    return (out_weight_grad,) + totals


def whole_kernel(
    sizes, heads, patch_width,
    shift_ref, qkv_ref, out_ref, cot_o, pat_o, emb_ref, embb_ref, gain_ref, bias_ref, rel_ref,
    grad_out, embed_out, bias_out, gain_out, table_out,
    qkv_all, out_all, cot_c, cot_r, cot_x, pat_c, pat_r, pat_x,
    pat_s, cot_s, xhat_s, inv_s, norm_s, proj_s, datt_s, att_s, dproj_s, bias_s, dtab_s, dn_s,
    gb, core_g, st, a1, b1, t2a, t2b, a2, b2, keep, zs, zr,
    small_s, core_e, es, er, fin,
    send_sem, recv_sem, own_sem, halo_send, halo_recv, red_send, red_recv,
    sml_send, sml_recv, all_send, all_recv, fwd_send, fwd_recv,
):
    bf16, f32, i32 = jnp.bfloat16, jnp.float32, jnp.int32
    rows, cols, dps = sizes
    row, col, dp = lax.axis_index("row"), lax.axis_index("col"), lax.axis_index("dp")
    x, z = row % 2, row // 2
    ring = rows // 2
    top = ring - 1
    core = (col + 1) % 2
    yes = row >= 0
    rows_dev, cols_dev, features = cot_o.shape
    edge = cot_c.shape[1]
    cells = WIN * WIN
    windows = cols_dev // WIN
    inner = att_s.shape[1]
    width = qkv_all.shape[3]
    groups = qkv_all.shape[0]
    out_width = out_all.shape[3]
    scale = (inner // heads) ** -0.5
    sr, sc = shift_ref[0, 0], shift_ref[0, 1]
    span = 2 * cells
    contract_last = (((1,), (1,)), ((), ()))
    contract_first = (((0,), (0,)), ((), ()))

    over_x = {"row": z * 2 + (x + 1) % 2}
    over_y = {"dp": (dp + 1) % 2}
    over_core = {"col": core}
    above_z = {"row": ((z + 1) % ring) * 2 + x}
    below_z = {"row": ((z + top) % ring) * 2 + x}

    def remote(source, target, send, recv, device):
        return pltpu.make_async_remote_copy(
            src_ref=source, dst_ref=target, send_sem=send, recv_sem=recv,
            device_id=device, device_id_type=MESH,
        )

    def flat(ref):
        return ref[...].reshape(-1, ref.shape[-1])

    barrier = pltpu.get_barrier_semaphore()
    others = 0
    for r in range(rows):
        for c in range(cols):
            for d in range(dps):
                if r or c or d:
                    others += 1
                    pl.semaphore_signal(
                        barrier, inc=1,
                        device_id={"row": (row + r) % rows, "col": (col + c) % cols, "dp": (dp + d) % dps},
                        device_id_type=MESH,
                    )
    for pair in range(heads // 2):
        one, two = bias_ref[2 * pair], bias_ref[2 * pair + 1]
        bias_s[pair] = jnp.concatenate([one, one, two, two], axis=1)
    pl.semaphore_wait(barrier, others)

    gathered, own = (qkv_all, out_all), (qkv_ref, out_ref)
    started = []

    def slot(a, flag, dy, dx, k):
        return gathered[a].at[((col + flag) % 2) * 2 + (dp + dy) % 2, k * 2 + (x + dx) % 2]

    def mark(a, flag, dy, dx, k):
        return recv_sem.at[a, ((flag * 2 + dy) * 2 + dx) * ring + k]

    def ship(a, dy, dx, k, device, landing, when, mine=False):
        target = slot(a, 0, dy, dx, k)
        copy = remote(
            own[a] if mine else target, target, send_sem.at[len(started)],
            mark(a, *landing, k), device,
        )
        started.append((copy, when))
        pl.when(when)(copy.start)

    def arrive(a, flag, dy, dx, k, when=yes):
        place = slot(a, flag, dy, dx, k)
        copy = remote(place, place, send_sem.at[0], mark(a, flag, dy, dx, k), over_core)
        pl.when(when)(copy.wait_recv)

    def to_core(a, dy, dx, k, when=yes, mine=False):
        ship(a, dy, dx, k, over_core, (1, dy, dx), when, mine)

    def own_line(a, k, when, up, down, mine=False):
        if up is not None:
            ship(a, 0, 0, k, above_z, (0, 0, 0), when & up, mine)
        if down is not None:
            ship(a, 0, 0, k, below_z, (0, 0, 0), when & down, mine)
        ship(a, 0, 0, k, over_y, (0, 1, 0), when, mine)
        ship(a, 0, 0, k, over_x, (0, 0, 1), when, mine)
        to_core(a, 0, 0, k, when, mine)

    can_up, can_down = z < top, z > 0
    near = z + 1 - 2 * (z % 2)
    low_half = z < ring // 2
    far = (jnp.where(low_half, 2, 1), jnp.where(low_half, 3, 0))

    def clamp(k):
        return jnp.minimum(jnp.maximum(k, 0), top)

    def line_step(a, j):
        below, over = z >= j, z + j <= top
        for k, ok, up, down in (
            (clamp(z - j), below, can_up, None), (clamp(z + j), over, None, can_down)
        ):
            arrive(a, 0, 0, 0, k, ok)
            own_line(a, k, ok, up if j < top else None, down if j < top else None)

    def x_near(a, k):
        arrive(a, 0, 0, 1, k)
        ship(a, 0, 1, k, over_y, (0, 1, 1), yes)
        to_core(a, 0, 1, k)

    def plain(a, dy, dx, k):
        arrive(a, 0, dy, dx, k)
        to_core(a, dy, dx, k)

    def diag_near(a, k):
        arrive(a, 0, 1, 1, k)
        ship(a, 1, 1, k, above_z, (0, 1, 1), z == 1)
        ship(a, 1, 1, k, below_z, (0, 1, 1), z == 2)
        to_core(a, 1, 1, k)

    def diag_far(a, k):
        arrive(a, 0, 1, 1, k)
        ship(a, 1, 1, k, above_z, (0, 1, 1), z == 2)
        ship(a, 1, 1, k, below_z, (0, 1, 1), z == 1)
        to_core(a, 1, 1, k)

    local = [
        pltpu.make_async_copy(own[a], slot(a, 0, 0, 0, z), own_sem.at[a]) for a in range(2)
    ]

    def stage0(a):
        own_line(a, z, yes, can_up, can_down, mine=True)
        local[a].start()

    def stage1(a):
        x_near(a, z)
        line_step(a, 1)
        plain(a, 1, 0, z)

    def stage2(a):
        diag_near(a, z)
        line_step(a, 2)
        x_near(a, near)
        plain(a, 1, 0, near)

    def stage3(a):
        line_step(a, 3)
        diag_near(a, near)
        for k in far:
            plain(a, 0, 1, k)
            plain(a, 1, 0, k)
            diag_far(a, k)

    def stage4(a):
        for dy in range(2):
            for dx in range(2):
                for k in range(ring):
                    arrive(a, 1, dy, dx, k)

    above, left = (row + rows - 1) % rows, (col + cols - 1) % cols
    short = rows_dev - 1
    halos = []

    def halo(source, target, device):
        copy = remote(source, target, halo_send.at[len(halos)], halo_recv.at[len(halos)], device)
        halos.append(copy)
        return copy

    pat_halos = [
        halo(pat_o.at[pl.ds(0, short)], pat_r, {"row": above}),
        halo(pat_o.at[pl.ds(0, short), pl.ds(0, edge)], pat_x, {"row": above, "col": left}),
        halo(pat_o.at[:, pl.ds(0, edge)], pat_c, {"col": left}),
    ]
    cot_side = halo(cot_o.at[:, pl.ds(0, edge)], cot_c, {"col": left})
    cot_down = halo(cot_o.at[pl.ds(0, short)], cot_r, {"row": above})
    cot_corner = halo(cot_r.at[:, pl.ds(0, edge)], cot_x, {"col": left})

    def picks_of(w):
        m = lax.broadcasted_iota(i32, (cells, 1), 0)
        r = (m // WIN) + sr
        c = w * WIN + (m % WIN) + sc
        up, before = r < rows_dev, c < cols_dev
        picks = []
        for ok, high_of, width_of, r_of, c_of in (
            (up & before, rows_dev, cols_dev, 0, 0),
            (up & ~before, rows_dev, edge, 0, cols_dev),
            (~up & before, short, cols_dev, rows_dev, 0),
            (~up & ~before, short, edge, rows_dev, cols_dev),
        ):
            place = jnp.where(ok, (r - r_of) * width_of + (c - c_of), -1)
            lanes = lax.broadcasted_iota(i32, (cells, high_of * width_of), 1)
            picks.append(jnp.where(lanes == place, 1.0, 0.0).astype(bf16))
        return picks

    def pick(picks, parts):
        got = None
        for one, ref in zip(picks, parts):
            term = jnp.dot(one, flat(ref), preferred_element_type=f32)
            got = term if got is None else got + term
        return got.astype(bf16)

    def prologue(w, carry):
        at = pl.ds(pl.multiple_of(w * cells, cells), cells)
        patch = pick(picks_of(w), (pat_o, pat_c, pat_r, pat_x))
        pat_s[at] = patch
        token = (
            jnp.dot(patch, emb_ref[...], preferred_element_type=f32) + embb_ref[...]
        ).astype(bf16).astype(f32)
        mean = jnp.mean(token, axis=-1, keepdims=True)
        centered = token - mean
        inv = lax.rsqrt(jnp.mean(centered * centered, axis=-1, keepdims=True) + norm_epsilon)
        xhat = centered * inv
        xhat_s[at] = xhat
        inv_s[at] = jnp.broadcast_to(inv, (cells, 128))
        norm_s[at] = (xhat * gain_ref[...]).astype(bf16)
        return carry

    def pick_cot(w, carry):
        at = pl.ds(pl.multiple_of(w * cells, cells), cells)
        cot_s[at] = pick(picks_of(w), (cot_o, cot_c, cot_r, cot_x))
        return carry

    def project():
        for g in range(groups):
            proj_s[:, g * width : (g + 1) * width] = jnp.dot(
                norm_s[...], flat(qkv_all.at[g]), preferred_element_type=f32
            ).astype(bf16)

    def attended_cot():
        datt = None
        for g in range(groups):
            term = lax.dot_general(
                cot_s[:, g * out_width : (g + 1) * out_width], flat(out_all.at[g]),
                contract_last, preferred_element_type=f32,
            )
            datt = term if datt is None else datt + term
        datt_s[...] = datt.astype(bf16)

    def mask_of(wp):
        m = lax.broadcasted_iota(i32, (span, 1), 0)
        n = lax.broadcasted_iota(i32, (1, 2 * span), 1) % span

        def label(cell):
            win = cell // cells
            r = row * rows_dev + (cell % cells) // WIN
            c = col * cols_dev + (wp * 2 + win) * WIN + cell % WIN
            down = (r >= rows * rows_dev - sr).astype(i32)
            over = (c >= cols * cols_dev - sc).astype(i32)
            return win * 4 + down * 2 + over

        return label(m) == label(n)

    masks = [mask_of(wp) for wp in range(windows // 2)]
    first = lax.broadcasted_iota(i32, (span, span), 1) < cells
    zero = jnp.zeros((span, span), bf16)

    def attend(hp, carry):
        at = pl.multiple_of(hp * span, span)
        bias = bias_s[hp]
        bias = jnp.concatenate([bias, bias], axis=0)
        kept = None
        for wp in range(windows // 2):
            rs = slice(wp * span, (wp + 1) * span)
            q = proj_s[rs, pl.ds(at, span)]
            k = proj_s[rs, pl.ds(inner + at, span)]
            v = proj_s[rs, pl.ds(2 * inner + at, span)]
            do = datt_s[rs, pl.ds(at, span)]
            ks = jnp.concatenate([jnp.where(first, k, zero), jnp.where(first, zero, k)], axis=0)
            vs = jnp.concatenate([jnp.where(first, v, zero), jnp.where(first, zero, v)], axis=0)
            s = lax.dot_general(q, ks, contract_last, preferred_element_type=f32)
            s = jnp.where(masks[wp], s * scale + bias, -1e30)
            dprob = lax.dot_general(do, vs, contract_last, preferred_element_type=f32)
            ps, dss = [], []
            for half in range(2):
                part = s[:, half * span : (half + 1) * span]
                e = jnp.exp(part - jnp.max(part, axis=-1, keepdims=True))
                p = e * (1.0 / jnp.sum(e, axis=-1, keepdims=True))
                d = dprob[:, half * span : (half + 1) * span]
                dss.append(p * (d - jnp.sum(p * d, axis=-1, keepdims=True)))
                ps.append(p)
            p_low = jnp.concatenate(ps, axis=1).astype(bf16)
            ds = jnp.concatenate(dss, axis=1)
            d_low = ds.astype(bf16)
            tab = ds[:cells] + ds[cells:]
            kept = tab if kept is None else kept + tab
            att_s[rs, pl.ds(at, span)] = jnp.dot(p_low, vs, preferred_element_type=f32).astype(bf16)
            dv = lax.dot_general(p_low, do, contract_first, preferred_element_type=f32)
            dq = jnp.dot(d_low, ks, preferred_element_type=f32) * scale
            dk = lax.dot_general(d_low, q, contract_first, preferred_element_type=f32) * scale
            dproj_s[rs, pl.ds(at, span)] = dq.astype(bf16)
            dproj_s[rs, pl.ds(inner + at, span)] = jnp.where(first, dk[:span], dk[span:]).astype(bf16)
            dproj_s[rs, pl.ds(2 * inner + at, span)] = jnp.where(first, dv[:span], dv[span:]).astype(bf16)
        dtab_s[hp] = kept
        return carry

    def back_project():
        for g in range(groups):
            term = lax.dot_general(
                dproj_s[:, g * width : (g + 1) * width], flat(qkv_all.at[g]),
                contract_last, preferred_element_type=f32,
            )
            if g == 0:
                dn_s[...] = term
            else:
                dn_s[...] += term

    def finish(w, gain_sum):
        at = pl.ds(pl.multiple_of(w * cells, cells), cells)
        dn = dn_s[at]
        xhat = xhat_s[at]
        gain_sum = gain_sum + jnp.sum(dn * xhat, axis=0, keepdims=True)
        g_rows = dn * gain_ref[...]
        mean = jnp.mean(g_rows, axis=-1, keepdims=True)
        along = jnp.mean(g_rows * xhat, axis=-1, keepdims=True)
        norm_s[at] = (inv_s[at][:, :1] * (g_rows - mean - xhat * along)).astype(bf16)
        return gain_sum

    entries = lax.broadcasted_iota(i32, (256, 2 * span), 0)

    def table_step(i, carry):
        for u in range(4):
            at = i * 4 + u
            spread = jnp.where(entries == rel_ref[pl.ds(at, 1), :], 1.0, 0.0).astype(bf16)
            one, two = dtab_s[:, at * 2, :], dtab_s[:, at * 2 + 1, :]
            part = jnp.concatenate(
                [
                    jnp.concatenate([one[:, :span], two[:, :span]], axis=1),
                    jnp.concatenate([one[:, span:], two[:, span:]], axis=1),
                ],
                axis=0,
            )
            high = part.astype(bf16).astype(f32)
            both = jnp.concatenate([high, part - high], axis=0).astype(bf16)
            carry = carry + lax.dot_general(both, spread, contract_last, preferred_element_type=f32)
        return carry

    pending = []

    def swap(index, source, target, device):
        copy = remote(source, target, red_send.at[index], red_recv.at[index], device)
        copy.start()
        pending.append(copy)
        return copy

    def grad_make():
        for g in range(groups):
            block = lax.dot_general(
                att_s[...], cot_s[:, g * out_width : (g + 1) * out_width],
                contract_first, preferred_element_type=f32,
            )
            gb[g] = block.astype(bf16).reshape(gb.shape[1:])
        return swap(0, gb.at[pl.ds(core * 2, 2)], core_g, over_core)

    half_rows = st.shape[4]

    def grad_first(got):
        got.wait_recv()
        for d in range(2):
            for r in range(rows):
                total = (gb[col * 2 + d, r].astype(f32) + core_g[d, r].astype(f32)).astype(bf16)
                st[0, d, r % 2, r // 2] = total[:half_rows]
                st[1, d, r % 2, r // 2] = total[half_rows:]
        return (
            swap(1, st.at[0, (dp + 1) % 2], a1, over_y),
            swap(2, st.at[1, :, (x + 1) % 2], b1, over_x),
        )

    def grad_second(got):
        for copy in got:
            copy.wait_recv()
        away, other = (x + 1) % 2, (dp + 1) % 2
        t2a[...] = (st[0, dp, away].astype(f32) + a1[away].astype(f32)).astype(bf16)
        t2b[...] = (st[1, other, x].astype(f32) + b1[other].astype(f32)).astype(bf16)
        sent = (swap(3, t2a, a2, over_x), swap(4, t2b, b2, over_y))
        keep[0] = st[0, dp, x].astype(f32) + a1[x].astype(f32)
        keep[1] = st[1, dp, x].astype(f32) + b1[dp].astype(f32)
        return sent

    def grad_third(got):
        for copy in got:
            copy.wait_recv()
        keep[0] += a2[...].astype(f32)
        keep[1] += b2[...].astype(f32)
        sent = []
        for s in range(1, ring):
            for h in range(2):
                zs[s, h] = keep[h, (z + s) % ring].astype(bf16)
            sent.append(swap(4 + s, zs.at[s], zr.at[s], {"row": ((z + s) % ring) * 2 + x}))
        return sent

    def grad_last(got):
        for copy in got:
            copy.wait_recv()
        for h in range(2):
            total = keep[h, z]
            for s in range(1, ring):
                total = total + zr[s, h].astype(f32)
            grad_out[h * half_rows : (h + 1) * half_rows] = total

    for copy in pat_halos:
        copy.start()
    stage0(0)
    cot_side.start()
    stage1(0)
    for copy in pat_halos:
        copy.wait_recv()
    lax.fori_loop(0, windows, prologue, 0)
    stage2(0)
    stage0(1)
    stage3(0)
    cot_down.start()
    stage1(1)
    stage4(0)
    local[0].wait()
    project()
    stage2(1)
    stage3(1)
    cot_down.wait_recv()
    cot_corner.start()
    stage4(1)
    local[1].wait()
    cot_side.wait_recv()
    cot_corner.wait_recv()
    lax.fori_loop(0, windows, pick_cot, 0)
    attended_cot()
    lax.fori_loop(0, heads // 2, attend, 0)
    got = grad_make()
    back_project()
    got = grad_first(got)
    tab = lax.fori_loop(0, cells // 8, table_step, jnp.zeros((2 * heads, 256), f32))
    tab = tab[:heads] + tab[heads:]
    got = grad_second(got)
    gain_sum = lax.fori_loop(0, windows, finish, jnp.zeros((1, features), f32))
    patch = pat_s[...]
    embed = lax.dot_general(patch, cot_s[...], contract_first, preferred_element_type=f32)
    embed = embed + lax.dot_general(patch, norm_s[...], contract_first, preferred_element_type=f32)
    depth = embed.shape[0]
    wide = features // cols
    for c in range(cols):
        for rg in range(depth // 8):
            for lh in range(wide // 256):
                at = c * wide + lh * 256
                small_s[c, rg * (wide // 256) + lh] = embed[rg * 8 : rg * 8 + 8, at : at + 256]
    per = wide // 256
    base = patch_width // 8
    for c in range(cols):
        for lh in range(per):
            at = c * wide + lh * 256
            small_s[c, base * per + lh, 1:2] = gain_sum[:, at : at + 256]
    small_s[0, base * per, 2:8] = tab[: heads // 2]
    small_s[0, (base + 1) * per, 0 : heads // 2] = tab[heads // 2 :]
    flip = remote(small_s.at[core], core_e, sml_send.at[0], sml_recv.at[0], over_core)
    flip.start()
    got = grad_third(got)
    flip.wait_recv()
    es[...] = small_s[col] + core_e[...]
    spread = []
    for r in range(rows):
        for d in range(dps):
            if r or d:
                to_row, to_dp = (row + r) % rows, (dp + d) % dps
                index = r * dps + d
                copy = remote(
                    es.at[to_row * dps + to_dp], er.at[index], sml_send.at[index], sml_recv.at[index],
                    {"row": to_row, "dp": to_dp},
                )
                copy.start()
                spread.append(copy)
    mine = row * dps + dp
    for copy in spread:
        copy.wait_recv()
    whole = es[mine]
    for index in range(1, rows * dps):
        whole = whole + er[index]
    fin[col, mine] = whole
    tell = []
    hand = remote(fin.at[col, mine], fin.at[col, mine], fwd_send.at[0], fwd_recv.at[0], over_core)
    for r in range(rows):
        for d in range(dps):
            if r or d:
                index = r * dps + d
                copy = remote(
                    fin.at[col, mine], fin.at[col, mine], all_send.at[index], all_recv.at[index],
                    {"row": (row + r) % rows, "dp": (dp + d) % dps},
                )
                copy.start()
                tell.append(copy)
    hand.start()
    grad_last(got)
    for r in range(rows):
        for d in range(dps):
            if r or d:
                index = r * dps + d
                part = ((row + rows - r) % rows) * dps + (dp + dps - d) % dps
                place = fin.at[col, part]
                remote(place, place, all_send.at[index], all_recv.at[index], over_core).wait_recv()
                copy = remote(place, place, fwd_send.at[index], fwd_recv.at[index], over_core)
                copy.start()
                tell.append(copy)
    for r in range(rows):
        for d in range(dps):
            index = r * dps + d
            part = ((row + rows - r) % rows) * dps + (dp + dps - d) % dps
            place = fin.at[core, part]
            remote(place, place, fwd_send.at[index], fwd_recv.at[index], over_core).wait_recv()
    for c in range(cols):
        for lh in range(per):
            at = c * wide + lh * 256
            for rg in range(base):
                embed_out[rg * 8 : rg * 8 + 8, at : at + 256] = fin[c, rg * per + lh]
            bias_out[:, at : at + 256] = fin[c, base * per + lh, 0:1]
            gain_out[:, at : at + 256] = fin[c, base * per + lh, 1:2]
    for i in range(heads // 2):
        table_out[2 * i : 2 * i + 1] = fin[0, base * per, 2 + i : 3 + i]
        table_out[2 * i + 1 : 2 * i + 2] = fin[0, (base + 1) * per, i : i + 1]
    for copy, when in started:
        pl.when(when)(copy.wait_send)
    for copy in halos + pending + [flip] + spread + tell + [hand]:
        copy.wait_send()


def direct_device(
    sizes, pixels, cotangent, embed_weight, embed_bias, layer_norm_gain,
    qkv_weight, out_weight, bias_table, rel_index, shifts,
):
    rows, cols, dps = sizes
    ring = rows // 2
    heads, table_size = bias_table.shape
    patch_width, features = embed_weight.shape
    bf16, f32 = jnp.bfloat16, jnp.float32
    cot_block = cotangent[0]
    rows_dev, cols_dev, _ = cot_block.shape
    groups = cols * dps
    depth = 64
    cells = WIN * WIN
    patches = make_patches(pixels)[0]
    tail = jnp.zeros(patches.shape[:2] + (depth - patch_width,), bf16).at[:, :, 0].set(1)
    pat_block = jnp.concatenate([patches, tail], axis=2)
    selector = (
        rel_index.reshape(-1)[:, None] == jnp.arange(table_size, dtype=jnp.int32)[None, :]
    ).astype(f32)
    bias_full = jnp.dot(selector, bias_table.T, precision=lax.Precision.HIGHEST).T.reshape(
        heads, cells, cells
    )
    twice = jnp.concatenate([rel_index, rel_index], axis=1).reshape(cells // 2, 4 * cells)
    inner = out_weight.shape[0] * rows
    here = rows_dev * cols_dev
    big = out_weight.shape
    half = big[0] // 2
    dma = pltpu.SemaphoreType.DMA
    vmem = pl.BlockSpec(memory_space=VMEM)
    sums = (rows * dps, 8, 256)
    grad, embed, bias, gain, table = pl.pallas_call(
        functools.partial(whole_kernel, sizes, heads, patch_width),
        out_shape=[
            jax.ShapeDtypeStruct(big, f32),
            jax.ShapeDtypeStruct((patch_width, features), f32),
            jax.ShapeDtypeStruct((1, features), f32),
            jax.ShapeDtypeStruct((1, features), f32),
            jax.ShapeDtypeStruct((heads, 256), f32),
        ],
        in_specs=[pl.BlockSpec(memory_space=pltpu.SMEM)] + [vmem] * 9,
        out_specs=[vmem] * 5,
        scratch_shapes=[
            VMEM((groups, rows) + qkv_weight.shape, bf16),
            VMEM((groups, rows) + big, bf16),
            VMEM((rows_dev, WIN, features), bf16),
            VMEM((rows_dev - 1, cols_dev, features), bf16),
            VMEM((rows_dev - 1, WIN, features), bf16),
            VMEM((rows_dev, WIN, depth), bf16),
            VMEM((rows_dev - 1, cols_dev, depth), bf16),
            VMEM((rows_dev - 1, WIN, depth), bf16),
            VMEM((here, depth), bf16),
            VMEM((here, features), bf16),
            VMEM((here, features), f32),
            VMEM((here, 128), f32),
            VMEM((here, features), bf16),
            VMEM((here, 3 * inner), bf16),
            VMEM((here, inner), bf16),
            VMEM((here, inner), bf16),
            VMEM((here, 3 * inner), bf16),
            VMEM((heads // 2, cells, 4 * cells), f32),
            VMEM((heads // 2, cells, 4 * cells), f32),
            VMEM((here, features), f32),
            VMEM((groups, rows) + big, bf16),
            VMEM((2, rows) + big, bf16),
            VMEM((2, 2, 2, ring, half, big[1]), bf16),
            VMEM((2, ring, half, big[1]), bf16),
            VMEM((2, ring, half, big[1]), bf16),
            VMEM((ring, half, big[1]), bf16),
            VMEM((ring, half, big[1]), bf16),
            VMEM((ring, half, big[1]), bf16),
            VMEM((ring, half, big[1]), bf16),
            VMEM((2, ring, half, big[1]), f32),
            VMEM((ring, 2, half, big[1]), bf16),
            VMEM((ring, 2, half, big[1]), bf16),
            VMEM((cols,) + sums, f32),
            VMEM(sums, f32), VMEM(sums, f32), VMEM(sums, f32),
            VMEM((cols,) + sums, f32),
            dma((200,)), dma((2, 8 * ring)), dma((2,)), dma((6,)), dma((6,)),
            dma((8,)), dma((8,)),
            dma((rows * dps,)), dma((rows * dps,)), dma((rows * dps,)), dma((rows * dps,)),
            dma((rows * dps,)), dma((rows * dps,)),
        ],
        compiler_params=pltpu.CompilerParams(
            collective_id=0, has_side_effects=True, vmem_limit_bytes=60 * 2**20
        ),
        name="whole",
    )(
        shifts, qkv_weight, out_weight, cot_block, pat_block,
        jnp.pad(embed_weight, ((0, depth - patch_width), (0, 0))),
        embed_bias[None], layer_norm_gain[None], bias_full, twice,
    )
    return (grad, embed, bias[0], gain[0], table[:, :table_size])


def solution(mesh):
    sizes = tuple(mesh.shape[name] for name in ("row", "col", "dp"))
    direct = sizes[1:] == (2, 2) and sizes[0] == 8
    return jax.shard_map(
        functools.partial(direct_device if direct else on_device, sizes),
        mesh=mesh,
        in_specs=(
            P("dp", None, "row", "col"),
            P("dp", "row", "col", None),
            P(),
            P(),
            P(),
            P("row", ("col", "dp")),
            P("row", ("col", "dp")),
            P(),
            P(),
            P("dp", None),
        ),
        out_specs=(P("row", ("col", "dp")), P(), P(), P(), P()),
        check_vma=False,
    )
```

```python
import functools

import jax
import jax.numpy as jnp
from jax import lax
from jax.experimental import pallas as pl
from jax.experimental.pallas import tpu as pltpu
from jax.sharding import PartitionSpec as P

WIN = 8
PATCH = 4


norm_epsilon = 1e-05


def from_behind(value, axis, steps):
    count = lax.axis_size(axis)
    pairs = [(source, (source + steps) % count) for source in range(count)]
    return lax.ppermute(value, axis, pairs)


def make_patches(pixel_block):
    images, channels, pixel_rows, pixel_cols = pixel_block.shape
    grid_rows = pixel_rows // PATCH
    grid_cols = pixel_cols // PATCH
    shaped = pixel_block.reshape(images, channels, grid_rows, PATCH, grid_cols, PATCH)
    return shaped.transpose(0, 2, 4, 1, 3, 5).reshape(
        images, grid_rows, grid_cols, channels * PATCH * PATCH
    )


def embed_cells(patches, embed_weight, embed_bias):
    return (jnp.dot(patches, embed_weight, preferred_element_type=jnp.float32) + embed_bias).astype(
        jnp.bfloat16
    )


def window_split(block):
    rows_all, cols_all, features = block.shape
    shaped = block.reshape(rows_all // WIN, WIN, cols_all // WIN, WIN, features)
    return shaped.transpose(0, 2, 1, 3, 4).reshape(-1, WIN * WIN, features)


def window_join(windows, rows_all, cols_all):
    features = windows.shape[-1]
    shaped = windows.reshape(rows_all // WIN, cols_all // WIN, WIN, WIN, features)
    return shaped.transpose(0, 2, 1, 3, 4).reshape(rows_all, cols_all, features)

def attend_forward(cell_windows, labels, layer_norm_gain, qkv_full, bias_full):
    window_count, cell_count, features = cell_windows.shape
    head_count = bias_full.shape[0]
    inner_width = qkv_full.shape[1] // 3
    head_size = inner_width // head_count
    score_scale = head_size ** (-0.5)
    flat_rows = cell_windows.reshape(-1, features).astype(jnp.float32)
    average = jnp.mean(flat_rows, axis=-1, keepdims=True)
    centered_input = flat_rows - average
    inverse_deviation = lax.rsqrt(
        jnp.mean(centered_input * centered_input, axis=-1, keepdims=True) + norm_epsilon
    )
    standardized_rows = centered_input * inverse_deviation
    normalized_rows = (standardized_rows * layer_norm_gain).astype(jnp.bfloat16)
    projected = jnp.dot(normalized_rows, qkv_full, preferred_element_type=jnp.float32).astype(
        jnp.bfloat16
    )
    head_shape = (window_count, cell_count, head_count, head_size)
    query_rows = projected[:, :inner_width].reshape(head_shape)
    key_vectors = projected[:, inner_width : 2 * inner_width].reshape(head_shape)
    value_rows = projected[:, 2 * inner_width :].reshape(head_shape)
    scores = (
        jnp.einsum("wmhd,wnhd->whmn", query_rows, key_vectors, preferred_element_type=jnp.float32)
        * score_scale
        + bias_full[None]
    )
    same_region = labels[:, None, :, None] == labels[:, None, None, :]
    scores = jnp.where(same_region, scores, -1e30)
    row_peak = jnp.max(scores, axis=-1, keepdims=True)
    exp_scores = jnp.exp(scores - row_peak)
    attention_weights = exp_scores / jnp.sum(exp_scores, axis=-1, keepdims=True)
    reduced_probability = attention_weights.astype(jnp.bfloat16)
    attended = jnp.einsum(
        "whmn,wnhd->wmhd", reduced_probability, value_rows, preferred_element_type=jnp.float32
    ).astype(jnp.bfloat16)
    stored_residuals = (
        standardized_rows,
        inverse_deviation,
        query_rows,
        key_vectors,
        value_rows,
        attention_weights,
        reduced_probability,
    )
    return (stored_residuals, attended.reshape(-1, inner_width))


def attend_backward(stored_residuals, d_attended, layer_norm_gain, qkv_full):
    (
        standardized_rows,
        inverse_deviation,
        query_rows,
        key_vectors,
        value_rows,
        attention_weights,
        reduced_probability,
    ) = stored_residuals
    head_shape = query_rows.shape
    score_scale = head_shape[3] ** (-0.5)
    total_row_count = standardized_rows.shape[0]
    inner_width = head_shape[2] * head_shape[3]
    d_heads = d_attended.reshape(head_shape)
    d_prob = jnp.einsum("wmhd,wnhd->whmn", d_heads, value_rows, preferred_element_type=jnp.float32)
    d_values = jnp.einsum(
        "whmn,wmhd->wnhd", reduced_probability, d_heads, preferred_element_type=jnp.float32
    ).astype(jnp.bfloat16)
    d_scores = attention_weights * (
        d_prob - jnp.sum(attention_weights * d_prob, axis=-1, keepdims=True)
    )
    table_part = jnp.sum(d_scores, axis=0)
    d_low = d_scores.astype(jnp.bfloat16)
    d_queries = (
        jnp.einsum("whmn,wnhd->wmhd", d_low, key_vectors, preferred_element_type=jnp.float32)
        * score_scale
    ).astype(jnp.bfloat16)
    d_keys = (
        jnp.einsum("whmn,wmhd->wnhd", d_low, query_rows, preferred_element_type=jnp.float32)
        * score_scale
    ).astype(jnp.bfloat16)
    d_projected = jnp.concatenate(
        [
            d_queries.reshape(total_row_count, inner_width),
            d_keys.reshape(total_row_count, inner_width),
            d_values.reshape(total_row_count, inner_width),
        ],
        axis=1,
    )
    normalized_gradient = lax.dot_general(
        d_projected, qkv_full, (((1,), (1,)), ((), ())), preferred_element_type=jnp.float32
    )
    gain_contribution = jnp.sum(normalized_gradient * standardized_rows, axis=0)
    scaled_rows = normalized_gradient * layer_norm_gain
    branch_gradient = inverse_deviation * (
        scaled_rows
        - jnp.mean(scaled_rows, axis=-1, keepdims=True)
        - standardized_rows * jnp.mean(scaled_rows * standardized_rows, axis=-1, keepdims=True)
    )
    return (branch_gradient.astype(jnp.bfloat16), gain_contribution, table_part)


MESH = pl.DeviceIdType.MESH
VMEM = pltpu.VMEM


def on_device(
    sizes,
    pixels,
    cotangent,
    embed_weight,
    embed_bias,
    layer_norm_gain,
    qkv_weight,
    out_weight,
    bias_table,
    rel_index,
    shifts,
):
    images, rows_dev, cols_dev, features = cotangent.shape
    rows, cols, dps = sizes
    head_count, table_size = bias_table.shape
    pix_block, cot_block = pixels[0], cotangent[0]
    row_shift, col_shift = shifts[0, 0], shifts[0, 1]
    qkv_full, out_full = [
        lax.all_gather(
            lax.all_gather(w, "row", axis=0, tiled=True), ("col", "dp"), axis=1, tiled=True
        )
        for w in (qkv_weight, out_weight)
    ]
    pix_r, cot_r = from_behind((pix_block, cot_block), "row", -1)
    pix_c, cot_c = from_behind((pix_block, cot_block[:, :WIN]), "col", -1)
    pix_x, cot_x = from_behind((pix_c, cot_c), "row", -1)
    wide_pix = jnp.concatenate(
        [
            jnp.concatenate([pix_block, pix_c[:, :, : WIN * PATCH]], axis=2),
            jnp.concatenate([pix_r, pix_x[:, :, : WIN * PATCH]], axis=2),
        ],
        axis=1,
    )
    wide_cot = jnp.concatenate(
        [
            jnp.concatenate([cot_block, cot_c], axis=1),
            jnp.concatenate([cot_r, cot_x], axis=1),
        ],
        axis=0,
    )
    wide_patches = make_patches(wide_pix[None])[0]
    patches = lax.dynamic_slice(
        wide_patches, (row_shift, col_shift, 0), (rows_dev, cols_dev, wide_patches.shape[2])
    )
    shifted_cot = lax.dynamic_slice(
        wide_cot, (row_shift, col_shift, 0), (rows_dev, cols_dev, features)
    )
    patch_rows = window_split(patches).reshape(-1, patches.shape[2])
    cot_flat = window_split(shifted_cot).reshape(-1, features)
    grid_rows, grid_cols = rows_dev * rows, cols_dev * cols
    row_ids = lax.axis_index("row") * rows_dev + jnp.arange(rows_dev, dtype=jnp.int32)
    col_ids = lax.axis_index("col") * cols_dev + jnp.arange(cols_dev, dtype=jnp.int32)
    row_part = (row_ids >= grid_rows - row_shift).astype(jnp.int32)
    col_part = (col_ids >= grid_cols - col_shift).astype(jnp.int32)
    region = 2 * row_part[:, None] + col_part[None, :]
    labels = window_split(region[:, :, None])[:, :, 0]
    selector = (
        rel_index.reshape(-1)[:, None] == jnp.arange(table_size, dtype=jnp.int32)[None, :]
    ).astype(jnp.float32)
    bias_full = jnp.dot(selector, bias_table.T, precision=lax.Precision.HIGHEST).T.reshape(
        head_count, WIN * WIN, WIN * WIN
    )
    cells = embed_cells(patch_rows, embed_weight, embed_bias)
    stored_residuals, attended = attend_forward(
        cells.reshape(-1, WIN * WIN, features), labels, layer_norm_gain, qkv_full, bias_full
    )
    d_attended = lax.dot_general(
        cot_flat, out_full, (((1,), (1,)), ((), ())), preferred_element_type=jnp.float32
    ).astype(jnp.bfloat16)
    d_rows, gain_contribution, table_part = attend_backward(
        stored_residuals, d_attended, layer_norm_gain, qkv_full
    )
    table_grad = jnp.dot(
        table_part.reshape(head_count, -1), selector, precision=lax.Precision.HIGHEST
    )
    contract = (((0,), (0,)), ((), ()))
    back_rows = jnp.concatenate([cot_flat, d_rows], axis=0)
    embed_grad = lax.dot_general(
        jnp.concatenate([patch_rows, patch_rows], axis=0),
        back_rows,
        contract,
        preferred_element_type=jnp.float32,
    )
    bias_grad = jnp.sum(back_rows, axis=0, dtype=jnp.float32)
    partial_rows = lax.psum_scatter(
        lax.dot_general(attended, cot_flat, contract, preferred_element_type=jnp.float32),
        "row",
        scatter_dimension=0,
        tiled=True,
    )
    out_weight_grad = lax.psum_scatter(
        partial_rows, ("col", "dp"), scatter_dimension=1, tiled=True
    )
    totals = lax.psum(
        (embed_grad, bias_grad, gain_contribution, table_grad), ("row", "col", "dp")
    )
    return (out_weight_grad,) + totals


UNROLL = 6


def whole_kernel(
    sizes, heads, patch_width,
    shift_ref, qkv_ref, out_ref, cot_ref, pix_ref, emb_ref, embb_ref, gain_ref, tab_ref, rel_ref,
    grad_out, embed_out, bias_out, gain_out, table_out,
    qkv_all, out_all, cot_o, pat_o, rel_s, bias_t, p_s, cot_c, cot_r, cot_x, pat_c, pat_r, pat_x,
    pat_s, cot_s, xhat_s, inv_s, norm_s, proj_s, datt_s, att_s, dproj_s, bias_s, dtab_s, dn_s,
    gb, core_g, st, a1, b1, t2a, t2b, a2, b2, keep, zs, zr,
    small_s, core_e, es, er, fin,
    send_sem, recv_sem, own_sem, halo_send, halo_recv, red_send, red_recv,
    sml_send, sml_recv, all_send, all_recv, fwd_send, fwd_recv,
):
    bf16, f32, i32 = jnp.bfloat16, jnp.float32, jnp.int32
    rows, cols, dps = sizes
    row, col, dp = lax.axis_index("row"), lax.axis_index("col"), lax.axis_index("dp")
    x, z = row % 2, row // 2
    ring = rows // 2
    top = ring - 1
    core = (col + 1) % 2
    yes = row >= 0
    rows_dev, cols_dev, features = cot_o.shape
    edge = cot_c.shape[1]
    cells = WIN * WIN
    windows = cols_dev // WIN
    inner = att_s.shape[1]
    chip_rows = qkv_all.shape[3]
    groups = qkv_all.shape[0]
    out_width = out_all.shape[3]
    scale = (inner // heads) ** -0.5
    sr, sc = shift_ref[0, 0], shift_ref[0, 1]
    span = 2 * cells
    contract_last = (((1,), (1,)), ((), ()))
    contract_first = (((0,), (0,)), ((), ()))

    over_x = {"row": z * 2 + (x + 1) % 2}
    over_y = {"dp": (dp + 1) % 2}
    over_core = {"col": core}
    above_z = {"row": ((z + 1) % ring) * 2 + x}
    below_z = {"row": ((z + top) % ring) * 2 + x}

    def remote(source, target, send, recv, device):
        return pltpu.make_async_remote_copy(
            src_ref=source, dst_ref=target, send_sem=send, recv_sem=recv,
            device_id=device, device_id_type=MESH,
        )

    def flat(ref):
        return ref[...].reshape(-1, ref.shape[-1])

    barrier = pltpu.get_barrier_semaphore()
    others = 0
    for r in range(rows):
        for c in range(cols):
            for d in range(dps):
                if r or c or d:
                    others += 1
                    pl.semaphore_signal(
                        barrier, inc=1,
                        device_id={"row": (row + r) % rows, "col": (col + c) % cols, "dp": (dp + d) % dps},
                        device_id_type=MESH,
                    )
    local = [
        pltpu.make_async_copy(source, target, own_sem.at[i])
        for i, (source, target) in enumerate(
            (
                (qkv_ref, qkv_all.at[col * 2 + dp, row]),
                (out_ref, out_all.at[col * 2 + dp, row]),
                (cot_ref.at[0], cot_o),
            )
        )
    ]
    for copy in local:
        copy.start()
    pl.semaphore_wait(barrier, others)

    def patchify():
        depth = pat_o.shape[2]
        channels, pixel_rows, pixel_cols = pix_ref.shape[1:]
        pix = pix_ref[0].reshape(channels * pixel_rows, pixel_cols)
        area = PATCH * PATCH
        f = lax.broadcasted_iota(i32, (depth, 1), 0)
        source_row = jnp.where(f < patch_width, (f // area) * pixel_rows + (f % area) // PATCH, -1024)
        row_lane = lax.broadcasted_iota(i32, (depth, channels * pixel_rows), 1)
        column = lax.broadcasted_iota(i32, (depth, pixel_cols), 1) % PATCH
        spot = lax.broadcasted_iota(i32, (cols_dev, pixel_cols), 1) // PATCH
        join = jnp.where(spot == lax.broadcasted_iota(i32, (cols_dev, pixel_cols), 0), 1.0, 0.0).astype(bf16)
        last = lax.broadcasted_iota(i32, (cols_dev, depth), 1) == patch_width
        for i in range(rows_dev):
            choose = jnp.where(row_lane == source_row + i * PATCH, 1.0, 0.0).astype(bf16)
            wide = jnp.dot(choose, pix, preferred_element_type=f32)
            wide = jnp.where(column == f % PATCH, wide, 0.0).astype(bf16)
            cell = lax.dot_general(join, wide, contract_last, preferred_element_type=f32)
            pat_o[i] = jnp.where(last, 1.0, cell).astype(bf16)
        rel_s[...] = jnp.concatenate([rel_ref[...], rel_ref[...]], axis=1)

    started = []
    parts = 2
    step = qkv_all.shape[2] // parts
    last_a = parts

    def slot(a, flag, dy, dx, k):
        which = ((col + flag) % 2) * 2 + (dp + dy) % 2, k * 2 + (x + dx) % 2
        if a == last_a:
            return out_all.at[which]
        return qkv_all.at[which[0], which[1], pl.ds(a * step, step)]

    def mark(a, flag, dy, dx, k):
        return recv_sem.at[a, ((flag * 2 + dy) * 2 + dx) * ring + k]

    def ship(a, dy, dx, k, device, landing, when):
        target = slot(a, 0, dy, dx, k)
        copy = remote(target, target, send_sem.at[len(started)], mark(a, *landing, k), device)
        started.append((copy, when))
        pl.when(when)(copy.start)

    def arrive(a, flag, dy, dx, k, when):
        place = slot(a, flag, dy, dx, k)
        copy = remote(place, place, send_sem.at[0], mark(a, flag, dy, dx, k), over_core)
        pl.when(when)(copy.wait_recv)

    can_up, can_down = z < top, z > 0
    middle = (z == 1) | (z == 2)

    def clamp(k):
        return jnp.minimum(jnp.maximum(k, 0), top)

    def around(j):
        if j == 0:
            return ((z, yes, 0),)
        return ((clamp(z - j), z >= j, 1), (clamp(z + j), z + j <= top, -1))

    def spread_own(a, k, when, way, j):
        if way >= 0 and j < top:
            ship(a, 0, 0, k, above_z, (0, 0, 0), when & can_up)
        if way <= 0 and j < top:
            ship(a, 0, 0, k, below_z, (0, 0, 0), when & can_down)
        ship(a, 0, 0, k, over_y, (0, 1, 0), when)
        ship(a, 0, 0, k, over_x, (0, 0, 1), when)
        ship(a, 0, 0, k, over_core, (1, 0, 0), when)

    def line(a, j):
        for k, when, way in around(j):
            arrive(a, 0, 0, 0, k, when)
            spread_own(a, k, when, way, j)

    def x_line(a, j):
        for k, when, _ in around(j):
            arrive(a, 0, 0, 1, k, when)
            if a == last_a:
                ship(a, 0, 1, k, over_y, (0, 1, 1), when)
            elif j == 0:
                ship(a, 0, 1, k, over_y, (0, 1, 1), when)
            ship(a, 0, 1, k, over_core, (1, 0, 1), when)

    def y_line(a, j):
        for k, when, _ in around(j):
            arrive(a, 0, 1, 0, k, when)
            if a != last_a and j == 1:
                ship(a, 1, 0, k, over_x, (0, 1, 1), when & (k // 2 == z // 2))
            ship(a, 1, 0, k, over_core, (1, 1, 0), when)

    def diagonal(a, j):
        for k, when, _ in around(j):
            arrive(a, 0, 1, 1, k, when)
            if a != last_a and j < 3:
                ship(a, 1, 1, k, above_z, (0, 1, 1), when & middle & (k < 2))
                ship(a, 1, 1, k, below_z, (0, 1, 1), when & middle & (k >= 2))
            ship(a, 1, 1, k, over_core, (1, 1, 1), when)

    def hop(a, h):
        if h == 0:
            spread_own(a, z, yes, 0, 0)
            return
        if h < ring:
            line(a, h)
        if h <= ring:
            x_line(a, h - 1)
        if 2 <= h <= ring + 1:
            diagonal(a, h - 2)
        if h <= ring:
            y_line(a, h - 1)

    def partner(a):
        for dy in range(2):
            for dx in range(2):
                for k in range(ring):
                    arrive(a, 1, dy, dx, k, yes)

    above, left = (row + rows - 1) % rows, (col + cols - 1) % cols
    short = rows_dev - 1
    halos = []

    def halo(source, target, device):
        copy = remote(source, target, halo_send.at[len(halos)], halo_recv.at[len(halos)], device)
        halos.append(copy)
        return copy

    pat_halos = [
        halo(pat_o.at[pl.ds(0, short)], pat_r, {"row": above}),
        halo(pat_o.at[pl.ds(0, short), pl.ds(0, edge)], pat_x, {"row": above, "col": left}),
        halo(pat_o.at[:, pl.ds(0, edge)], pat_c, {"col": left}),
    ]
    cot_side = halo(cot_o.at[:, pl.ds(0, edge)], cot_c, {"col": left})
    cuts = [(r, min(2, short - r)) for r in range(0, short, 2)]
    cot_down = [
        halo(cot_o.at[pl.ds(r, n)], cot_r.at[pl.ds(r, n)], {"row": above}) for r, n in cuts
    ]
    cot_corner = halo(cot_r.at[:, pl.ds(0, edge)], cot_x, {"col": left})

    def picks_of(w):
        m = lax.broadcasted_iota(i32, (cells, 1), 0)
        r = (m // WIN) + sr
        c = w * WIN + (m % WIN) + sc
        up, before = r < rows_dev, c < cols_dev
        picks = []
        for ok, high_of, width_of, r_of, c_of in (
            (up & before, rows_dev, cols_dev, 0, 0),
            (up & ~before, rows_dev, edge, 0, cols_dev),
            (~up & before, short, cols_dev, rows_dev, 0),
            (~up & ~before, short, edge, rows_dev, cols_dev),
        ):
            place = jnp.where(ok, (r - r_of) * width_of + (c - c_of), -1)
            lanes = lax.broadcasted_iota(i32, (cells, high_of * width_of), 1)
            picks.append(jnp.where(lanes == place, 1.0, 0.0).astype(bf16))
        return picks

    def pick(picks, parts):
        got = None
        for one, ref in zip(picks, parts):
            term = jnp.dot(one, flat(ref), preferred_element_type=f32)
            got = term if got is None else got + term
        return got.astype(bf16)

    def prologue(w, carry):
        at = pl.ds(pl.multiple_of(w * cells, cells), cells)
        patch = pick(picks_of(w), (pat_o, pat_c, pat_r, pat_x))
        pat_s[at] = patch
        token = (
            jnp.dot(patch[:, :patch_width], emb_ref[...], preferred_element_type=f32) + embb_ref[...]
        ).astype(bf16).astype(f32)
        mean = jnp.mean(token, axis=-1, keepdims=True)
        centered = token - mean
        inv = lax.rsqrt(jnp.mean(centered * centered, axis=-1, keepdims=True) + norm_epsilon)
        xhat = centered * inv
        xhat_s[at] = xhat
        inv_s[at] = jnp.broadcast_to(inv, (cells, 128))
        norm_s[at] = (xhat * gain_ref[...]).astype(bf16)
        return carry

    def pick_cot(w, carry):
        at = pl.ds(pl.multiple_of(w * cells, cells), cells)
        cot_s[at] = pick(picks_of(w), (cot_o, cot_c, cot_r, cot_x))
        return carry

    def weight_rows(r):
        return jnp.concatenate([qkv_all[g, r] for g in range(groups)], axis=0)

    def project():
        full = jnp.concatenate([weight_rows(r) for r in range(rows)], axis=1)
        for n in range(0, 3 * inner, inner):
            proj_s[:, n : n + inner] = lax.dot_general(
                norm_s[...], full[n : n + inner], contract_last, preferred_element_type=f32
            ).astype(bf16)

    def attended_cot():
        datt = None
        for g in range(groups):
            term = lax.dot_general(
                cot_s[:, g * out_width : (g + 1) * out_width], flat(out_all.at[g]),
                contract_last, preferred_element_type=f32,
            )
            datt = term if datt is None else datt + term
        datt_s[...] = datt.astype(bf16)

    def mask_of(wp):
        m = lax.broadcasted_iota(i32, (span, 1), 0)
        n = lax.broadcasted_iota(i32, (1, 2 * span), 1) % span

        def label(cell):
            win = cell // cells
            r = row * rows_dev + (cell % cells) // WIN
            c = col * cols_dev + (wp * 2 + win) * WIN + cell % WIN
            down = (r >= rows * rows_dev - sr).astype(i32)
            over = (c >= cols * cols_dev - sc).astype(i32)
            return win * 4 + down * 2 + over

        return label(m) == label(n)

    masks = [mask_of(wp) for wp in range(windows // 2)]
    first = lax.broadcasted_iota(i32, (span, span), 1) < cells
    zero = jnp.zeros((span, span), bf16)

    def stacked(value):
        return jnp.concatenate([jnp.where(first, value, zero), jnp.where(first, zero, value)], axis=0)

    def attend(hp, carry):
        at = pl.multiple_of(hp * span, span)
        bias = bias_s[hp]
        bias = jnp.concatenate([bias, bias], axis=0)
        for wp in range(windows // 2):
            rs = slice(wp * span, (wp + 1) * span)
            q = proj_s[rs, pl.ds(at, span)]
            ks = stacked(proj_s[rs, pl.ds(inner + at, span)])
            vs = stacked(proj_s[rs, pl.ds(2 * inner + at, span)])
            s = lax.dot_general(q, ks, contract_last, preferred_element_type=f32)
            s = jnp.where(masks[wp], s * scale + bias, -1e30)
            ps = []
            for half in range(2):
                part = s[:, half * span : (half + 1) * span]
                e = jnp.exp(part - jnp.max(part, axis=-1, keepdims=True))
                ps.append(e * (1.0 / jnp.sum(e, axis=-1, keepdims=True)))
            p = jnp.concatenate(ps, axis=1)
            p_s[hp, wp] = p
            att_s[rs, pl.ds(at, span)] = jnp.dot(
                p.astype(bf16), vs, preferred_element_type=f32
            ).astype(bf16)
        return carry

    def attend_back(hp, carry):
        at = pl.multiple_of(hp * span, span)
        kept = None
        for wp in range(windows // 2):
            rs = slice(wp * span, (wp + 1) * span)
            q = proj_s[rs, pl.ds(at, span)]
            ks = stacked(proj_s[rs, pl.ds(inner + at, span)])
            vs = stacked(proj_s[rs, pl.ds(2 * inner + at, span)])
            do = datt_s[rs, pl.ds(at, span)]
            dprob = lax.dot_general(do, vs, contract_last, preferred_element_type=f32)
            p = p_s[hp, wp]
            dss = []
            for half in range(2):
                part = p[:, half * span : (half + 1) * span]
                d = dprob[:, half * span : (half + 1) * span]
                dss.append(part * (d - jnp.sum(part * d, axis=-1, keepdims=True)))
            p_low = p.astype(bf16)
            ds = jnp.concatenate(dss, axis=1)
            d_low = ds.astype(bf16)
            tab = ds[:cells] + ds[cells:]
            kept = tab if kept is None else kept + tab
            dv = lax.dot_general(p_low, do, contract_first, preferred_element_type=f32)
            dq = jnp.dot(d_low, ks, preferred_element_type=f32) * scale
            dk = lax.dot_general(d_low, q, contract_first, preferred_element_type=f32) * scale
            dproj_s[rs, pl.ds(at, span)] = dq.astype(bf16)
            dproj_s[rs, pl.ds(inner + at, span)] = jnp.where(first, dk[:span], dk[span:]).astype(bf16)
            dproj_s[rs, pl.ds(2 * inner + at, span)] = jnp.where(first, dv[:span], dv[span:]).astype(bf16)
        dtab_s[hp] = kept
        return carry

    def back_project():
        for r in range(0, rows, 2):
            two = jnp.concatenate([weight_rows(r), weight_rows(r + 1)], axis=1)
            dn_s[:, r * chip_rows : (r + 2) * chip_rows] = jnp.dot(
                dproj_s[...], two, preferred_element_type=f32
            )

    def finish(w, gain_sum):
        at = pl.ds(pl.multiple_of(w * cells, cells), cells)
        dn = dn_s[at]
        xhat = xhat_s[at]
        gain_sum = gain_sum + jnp.sum(dn * xhat, axis=0, keepdims=True)
        g_rows = dn * gain_ref[...]
        mean = jnp.mean(g_rows, axis=-1, keepdims=True)
        along = jnp.mean(g_rows * xhat, axis=-1, keepdims=True)
        norm_s[at] = (inv_s[at][:, :1] * (g_rows - mean - xhat * along)).astype(bf16)
        return gain_sum

    entries = lax.broadcasted_iota(i32, (256, 2 * span), 0)

    def spread_of(at):
        pair = jnp.concatenate([rel_s[pl.ds(2 * at, 1), :], rel_s[pl.ds(2 * at + 1, 1), :]], axis=1)
        return jnp.where(entries == pair, 1.0, 0.0).astype(bf16)

    def bias_make(start, stop, final):
        order = [tab_ref[i : i + 1, :] for i in list(range(0, heads, 2)) + list(range(1, heads, 2))]
        rest = jnp.concatenate(order, axis=0)
        rest = jnp.concatenate(
            [rest, jnp.zeros((heads, 256 - rest.shape[1]), f32)], axis=1
        )
        terms = []
        for _ in range(3):
            low = rest.astype(bf16)
            terms.append(low)
            rest = rest - low.astype(f32)
        stack = jnp.concatenate([t.astype(f32) for t in terms], axis=0).astype(bf16)

        def one(i, carry):
            for u in range(4):
                at = i * 4 + u
                got = jnp.dot(stack, spread_of(at), preferred_element_type=f32)
                got = got[:heads] + got[heads : 2 * heads] + got[2 * heads :]
                for v in range(2):
                    piece = got[:, v * span : (v + 1) * span]
                    m = 2 * at + v
                    bias_t[m, : heads // 2, :span] = piece[: heads // 2]
                    bias_t[m, : heads // 2, span:] = piece[heads // 2 :]
            return carry

        lax.fori_loop(start, stop, one, 0)
        for pair in range(heads // 2 if final else 0):
            bias_s[pair] = bias_t[:, pair, :]

    def table_step(i, carry):
        for u in range(4):
            at = i * 4 + u
            one, two = dtab_s[:, at * 2, :], dtab_s[:, at * 2 + 1, :]
            part = jnp.concatenate(
                [
                    jnp.concatenate([one[:, :span], two[:, :span]], axis=1),
                    jnp.concatenate([one[:, span:], two[:, span:]], axis=1),
                ],
                axis=0,
            )
            high = part.astype(bf16).astype(f32)
            both = jnp.concatenate([high, part - high], axis=0).astype(bf16)
            carry = carry + lax.dot_general(
                both, spread_of(at), contract_last, preferred_element_type=f32
            )
        return carry

    pending = []

    def swap(index, source, target, device):
        copy = remote(source, target, red_send.at[index], red_recv.at[index], device)
        copy.start()
        pending.append(copy)
        return copy

    def grad_make():
        for g in range(groups):
            block = lax.dot_general(
                att_s[...], cot_s[:, g * out_width : (g + 1) * out_width],
                contract_first, preferred_element_type=f32,
            )
            gb[g] = block.astype(bf16).reshape(gb.shape[1:])
        return swap(0, gb.at[pl.ds(core * 2, 2)], core_g, over_core)

    half_rows = st.shape[4]

    def grad_first(got):
        got.wait_recv()
        for d in range(2):
            for r in range(rows):
                total = (gb[col * 2 + d, r].astype(f32) + core_g[d, r].astype(f32)).astype(bf16)
                st[0, d, r % 2, r // 2] = total[:half_rows]
                st[1, d, r % 2, r // 2] = total[half_rows:]
        return (
            swap(1, st.at[0, (dp + 1) % 2], a1, over_y),
            swap(2, st.at[1, :, (x + 1) % 2], b1, over_x),
        )

    def grad_second(got):
        for copy in got:
            copy.wait_recv()
        away, other = (x + 1) % 2, (dp + 1) % 2
        t2a[...] = (st[0, dp, away].astype(f32) + a1[away].astype(f32)).astype(bf16)
        t2b[...] = (st[1, other, x].astype(f32) + b1[other].astype(f32)).astype(bf16)
        sent = (swap(3, t2a, a2, over_x), swap(4, t2b, b2, over_y))
        keep[0] = st[0, dp, x].astype(f32) + a1[x].astype(f32)
        keep[1] = st[1, dp, x].astype(f32) + b1[dp].astype(f32)
        return sent

    def grad_third(got):
        for copy in got:
            copy.wait_recv()
        keep[0] += a2[...].astype(f32)
        keep[1] += b2[...].astype(f32)
        sent = []
        for s in range(1, ring):
            for h in range(2):
                zs[s, h] = keep[h, (z + s) % ring].astype(bf16)
            sent.append(swap(4 + s, zs.at[s], zr.at[s], {"row": ((z + s) % ring) * 2 + x}))
        return sent

    def grad_last(got):
        for copy in got:
            copy.wait_recv()
        for h in range(2):
            total = keep[h, z]
            for s in range(1, ring):
                total = total + zr[s, h].astype(f32)
            grad_out[h * half_rows : (h + 1) * half_rows] = total

    def unrolled(body):
        def several(i, carry):
            for u in range(UNROLL):
                body(i * UNROLL + u, carry)
            return carry

        lax.fori_loop(0, heads // 2 // UNROLL, several, 0)

    local[0].wait()
    local[1].wait()
    every = parts + 1

    def hops(h):
        for a in range(every):
            hop(a, h)

    hops(0)
    patchify()
    for copy in pat_halos:
        copy.start()
    local[2].wait()
    cot_side.start()
    cot_down[0].start()
    hops(1)
    bias_make(0, cells // 16, False)
    for copy in cot_down[1:-1]:
        copy.start()
    hops(2)
    for copy in pat_halos:
        copy.wait_recv()
    lax.fori_loop(0, windows // 2, prologue, 0)
    cot_down[-1].start()
    hops(3)
    lax.fori_loop(windows // 2, windows, prologue, 0)
    hops(4)
    bias_make(cells // 16, cells // 8, True)
    for copy in cot_down:
        copy.wait_recv()
    cot_corner.start()
    hops(5)
    cot_side.wait_recv()
    cot_corner.wait_recv()
    lax.fori_loop(0, windows, pick_cot, 0)
    for a in range(parts):
        partner(a)
    project()
    unrolled(attend)
    got = grad_make()
    partner(last_a)
    attended_cot()
    got = grad_first(got)
    unrolled(attend_back)
    got = grad_second(got)
    tab = lax.fori_loop(0, cells // 8, table_step, jnp.zeros((2 * heads, 256), f32))
    tab = tab[:heads] + tab[heads:]
    back_project()
    got = grad_third(got)
    gain_sum = lax.fori_loop(0, windows, finish, jnp.zeros((1, features), f32))
    patch = pat_s[...]
    embed = lax.dot_general(patch, cot_s[...], contract_first, preferred_element_type=f32)
    embed = embed + lax.dot_general(patch, norm_s[...], contract_first, preferred_element_type=f32)
    depth = embed.shape[0]
    wide = features // cols
    for c in range(cols):
        for rg in range(depth // 8):
            for lh in range(wide // 256):
                at = c * wide + lh * 256
                small_s[c, rg * (wide // 256) + lh] = embed[rg * 8 : rg * 8 + 8, at : at + 256]
    per = wide // 256
    base = patch_width // 8
    for c in range(cols):
        for lh in range(per):
            at = c * wide + lh * 256
            small_s[c, base * per + lh, 1:2] = gain_sum[:, at : at + 256]
    small_s[0, base * per, 2:8] = tab[: heads // 2]
    small_s[0, (base + 1) * per, 0 : heads // 2] = tab[heads // 2 :]
    flip = remote(small_s.at[core], core_e, sml_send.at[0], sml_recv.at[0], over_core)
    flip.start()
    flip.wait_recv()
    es[...] = small_s[col] + core_e[...]
    spread = []
    for r in range(rows):
        for d in range(dps):
            if r or d:
                to_row, to_dp = (row + r) % rows, (dp + d) % dps
                index = r * dps + d
                copy = remote(
                    es.at[to_row * dps + to_dp], er.at[index], sml_send.at[index], sml_recv.at[index],
                    {"row": to_row, "dp": to_dp},
                )
                copy.start()
                spread.append(copy)
    mine = row * dps + dp
    for copy in spread:
        copy.wait_recv()
    whole = es[mine]
    for index in range(1, rows * dps):
        whole = whole + er[index]
    fin[col, mine] = whole
    tell = []
    hand = remote(fin.at[col, mine], fin.at[col, mine], fwd_send.at[0], fwd_recv.at[0], over_core)
    for r in range(rows):
        for d in range(dps):
            if r or d:
                index = r * dps + d
                copy = remote(
                    fin.at[col, mine], fin.at[col, mine], all_send.at[index], all_recv.at[index],
                    {"row": (row + r) % rows, "dp": (dp + d) % dps},
                )
                copy.start()
                tell.append(copy)
    hand.start()
    grad_last(got)
    for r in range(rows):
        for d in range(dps):
            if r or d:
                index = r * dps + d
                part = ((row + rows - r) % rows) * dps + (dp + dps - d) % dps
                place = fin.at[col, part]
                remote(place, place, all_send.at[index], all_recv.at[index], over_core).wait_recv()
                copy = remote(place, place, fwd_send.at[index], fwd_recv.at[index], over_core)
                copy.start()
                tell.append(copy)
    for r in range(rows):
        for d in range(dps):
            index = r * dps + d
            part = ((row + rows - r) % rows) * dps + (dp + dps - d) % dps
            place = fin.at[core, part]
            remote(place, place, fwd_send.at[index], fwd_recv.at[index], over_core).wait_recv()
    for c in range(cols):
        for lh in range(per):
            at = c * wide + lh * 256
            for rg in range(base):
                embed_out[rg * 8 : rg * 8 + 8, at : at + 256] = fin[c, rg * per + lh]
            bias_out[:, at : at + 256] = fin[c, base * per + lh, 0:1]
            gain_out[:, at : at + 256] = fin[c, base * per + lh, 1:2]
    for i in range(heads // 2):
        table_out[2 * i : 2 * i + 1] = fin[0, base * per, 2 + i : 3 + i]
        table_out[2 * i + 1 : 2 * i + 2] = fin[0, (base + 1) * per, i : i + 1]
    for copy, when in started:
        pl.when(when)(copy.wait_send)
    for copy in halos + pending + [flip] + spread + tell + [hand]:
        copy.wait_send()


def direct_device(
    sizes, pixels, cotangent, embed_weight, embed_bias, layer_norm_gain,
    qkv_weight, out_weight, bias_table, rel_index, shifts,
):
    rows, cols, dps = sizes
    ring = rows // 2
    heads, table_size = bias_table.shape
    patch_width, features = embed_weight.shape
    bf16, f32 = jnp.bfloat16, jnp.float32
    _, rows_dev, cols_dev, _ = cotangent.shape
    groups = cols * dps
    depth = 64
    cells = WIN * WIN
    inner = out_weight.shape[0] * rows
    here = rows_dev * cols_dev
    big = out_weight.shape
    half = big[0] // 2
    dma = pltpu.SemaphoreType.DMA
    vmem = pl.BlockSpec(memory_space=VMEM)
    sums = (rows * dps, 8, 256)
    grad, embed, bias, gain, table = pl.pallas_call(
        functools.partial(whole_kernel, sizes, heads, patch_width),
        out_shape=[
            jax.ShapeDtypeStruct(big, f32),
            jax.ShapeDtypeStruct((patch_width, features), f32),
            jax.ShapeDtypeStruct((1, features), f32),
            jax.ShapeDtypeStruct((1, features), f32),
            jax.ShapeDtypeStruct((heads, 256), f32),
        ],
        in_specs=[pl.BlockSpec(memory_space=pltpu.SMEM)] + [pl.BlockSpec(memory_space=pl.ANY)] * 3 + [vmem] * 6,
        out_specs=[vmem] * 5,
        scratch_shapes=[
            VMEM((groups, rows) + qkv_weight.shape[::-1], bf16),
            VMEM((groups, rows) + big, bf16),
            VMEM((rows_dev, cols_dev, features), bf16),
            VMEM((rows_dev, cols_dev, depth), bf16),
            VMEM((cells, 2 * cells), jnp.int32),
            VMEM((cells, 8 * pl.cdiv(heads, 16), 4 * cells), f32),
            VMEM((heads // 2, cols_dev // (2 * WIN), 2 * cells, 4 * cells), f32),
            VMEM((rows_dev, WIN, features), bf16),
            VMEM((rows_dev - 1, cols_dev, features), bf16),
            VMEM((rows_dev - 1, WIN, features), bf16),
            VMEM((rows_dev, WIN, depth), bf16),
            VMEM((rows_dev - 1, cols_dev, depth), bf16),
            VMEM((rows_dev - 1, WIN, depth), bf16),
            VMEM((here, depth), bf16),
            VMEM((here, features), bf16),
            VMEM((here, features), f32),
            VMEM((here, 128), f32),
            VMEM((here, features), bf16),
            VMEM((here, 3 * inner), bf16),
            VMEM((here, inner), bf16),
            VMEM((here, inner), bf16),
            VMEM((here, 3 * inner), bf16),
            VMEM((heads // 2, cells, 4 * cells), f32),
            VMEM((heads // 2, cells, 4 * cells), f32),
            VMEM((here, features), f32),
            VMEM((groups, rows) + big, bf16),
            VMEM((2, rows) + big, bf16),
            VMEM((2, 2, 2, ring, half, big[1]), bf16),
            VMEM((2, ring, half, big[1]), bf16),
            VMEM((2, ring, half, big[1]), bf16),
            VMEM((ring, half, big[1]), bf16),
            VMEM((ring, half, big[1]), bf16),
            VMEM((ring, half, big[1]), bf16),
            VMEM((ring, half, big[1]), bf16),
            VMEM((2, ring, half, big[1]), f32),
            VMEM((ring, 2, half, big[1]), bf16),
            VMEM((ring, 2, half, big[1]), bf16),
            VMEM((cols,) + sums, f32),
            VMEM(sums, f32), VMEM(sums, f32), VMEM(sums, f32),
            VMEM((cols,) + sums, f32),
            dma((400,)), dma((3, 8 * ring)), dma((3,)), dma((16,)), dma((16,)),
            dma((8,)), dma((8,)),
            dma((rows * dps,)), dma((rows * dps,)), dma((rows * dps,)), dma((rows * dps,)),
            dma((rows * dps,)), dma((rows * dps,)),
        ],
        compiler_params=pltpu.CompilerParams(
            collective_id=0, has_side_effects=True, vmem_limit_bytes=60 * 2**20
        ),
        name="whole",
    )(
        shifts, qkv_weight.T, out_weight, cotangent, pixels, embed_weight,
        embed_bias[None], layer_norm_gain[None], bias_table, rel_index,
    )
    return (grad, embed, bias[0], gain[0], table[:, :table_size])


def solution(mesh):
    sizes = tuple(mesh.shape[name] for name in ("row", "col", "dp"))
    direct = sizes[1:] == (2, 2) and sizes[0] == 8
    return jax.shard_map(
        functools.partial(direct_device if direct else on_device, sizes),
        mesh=mesh,
        in_specs=(
            P("dp", None, "row", "col"),
            P("dp", "row", "col", None),
            P(),
            P(),
            P(),
            P("row", ("col", "dp")),
            P("row", ("col", "dp")),
            P(),
            P(),
            P("dp", None),
        ),
        out_specs=(P("row", ("col", "dp")), P(), P(), P(), P()),
        check_vma=False,
    )
```

```python
import functools

import jax
import jax.numpy as jnp
from jax import lax
from jax.experimental import pallas as pl
from jax.experimental.pallas import tpu as pltpu
from jax.sharding import PartitionSpec as P

WIN = 8
PATCH = 4


norm_epsilon = 1e-05


def from_behind(value, axis, steps):
    count = lax.axis_size(axis)
    pairs = [(source, (source + steps) % count) for source in range(count)]
    return lax.ppermute(value, axis, pairs)


def make_patches(pixel_block):
    images, channels, pixel_rows, pixel_cols = pixel_block.shape
    grid_rows = pixel_rows // PATCH
    grid_cols = pixel_cols // PATCH
    shaped = pixel_block.reshape(images, channels, grid_rows, PATCH, grid_cols, PATCH)
    return shaped.transpose(0, 2, 4, 1, 3, 5).reshape(
        images, grid_rows, grid_cols, channels * PATCH * PATCH
    )


def embed_cells(patches, embed_weight, embed_bias):
    return (jnp.dot(patches, embed_weight, preferred_element_type=jnp.float32) + embed_bias).astype(
        jnp.bfloat16
    )


def window_split(block):
    rows_all, cols_all, features = block.shape
    shaped = block.reshape(rows_all // WIN, WIN, cols_all // WIN, WIN, features)
    return shaped.transpose(0, 2, 1, 3, 4).reshape(-1, WIN * WIN, features)


def window_join(windows, rows_all, cols_all):
    features = windows.shape[-1]
    shaped = windows.reshape(rows_all // WIN, cols_all // WIN, WIN, WIN, features)
    return shaped.transpose(0, 2, 1, 3, 4).reshape(rows_all, cols_all, features)

def attend_forward(cell_windows, labels, layer_norm_gain, qkv_full, bias_full):
    window_count, cell_count, features = cell_windows.shape
    head_count = bias_full.shape[0]
    inner_width = qkv_full.shape[1] // 3
    head_size = inner_width // head_count
    score_scale = head_size ** (-0.5)
    flat_rows = cell_windows.reshape(-1, features).astype(jnp.float32)
    average = jnp.mean(flat_rows, axis=-1, keepdims=True)
    centered_input = flat_rows - average
    inverse_deviation = lax.rsqrt(
        jnp.mean(centered_input * centered_input, axis=-1, keepdims=True) + norm_epsilon
    )
    standardized_rows = centered_input * inverse_deviation
    normalized_rows = (standardized_rows * layer_norm_gain).astype(jnp.bfloat16)
    projected = jnp.dot(normalized_rows, qkv_full, preferred_element_type=jnp.float32).astype(
        jnp.bfloat16
    )
    head_shape = (window_count, cell_count, head_count, head_size)
    query_rows = projected[:, :inner_width].reshape(head_shape)
    key_vectors = projected[:, inner_width : 2 * inner_width].reshape(head_shape)
    value_rows = projected[:, 2 * inner_width :].reshape(head_shape)
    scores = (
        jnp.einsum("wmhd,wnhd->whmn", query_rows, key_vectors, preferred_element_type=jnp.float32)
        * score_scale
        + bias_full[None]
    )
    same_region = labels[:, None, :, None] == labels[:, None, None, :]
    scores = jnp.where(same_region, scores, -1e30)
    row_peak = jnp.max(scores, axis=-1, keepdims=True)
    exp_scores = jnp.exp(scores - row_peak)
    attention_weights = exp_scores / jnp.sum(exp_scores, axis=-1, keepdims=True)
    reduced_probability = attention_weights.astype(jnp.bfloat16)
    attended = jnp.einsum(
        "whmn,wnhd->wmhd", reduced_probability, value_rows, preferred_element_type=jnp.float32
    ).astype(jnp.bfloat16)
    stored_residuals = (
        standardized_rows,
        inverse_deviation,
        query_rows,
        key_vectors,
        value_rows,
        attention_weights,
        reduced_probability,
    )
    return (stored_residuals, attended.reshape(-1, inner_width))


def attend_backward(stored_residuals, d_attended, layer_norm_gain, qkv_full):
    (
        standardized_rows,
        inverse_deviation,
        query_rows,
        key_vectors,
        value_rows,
        attention_weights,
        reduced_probability,
    ) = stored_residuals
    head_shape = query_rows.shape
    score_scale = head_shape[3] ** (-0.5)
    total_row_count = standardized_rows.shape[0]
    inner_width = head_shape[2] * head_shape[3]
    d_heads = d_attended.reshape(head_shape)
    d_prob = jnp.einsum("wmhd,wnhd->whmn", d_heads, value_rows, preferred_element_type=jnp.float32)
    d_values = jnp.einsum(
        "whmn,wmhd->wnhd", reduced_probability, d_heads, preferred_element_type=jnp.float32
    ).astype(jnp.bfloat16)
    d_scores = attention_weights * (
        d_prob - jnp.sum(attention_weights * d_prob, axis=-1, keepdims=True)
    )
    table_part = jnp.sum(d_scores, axis=0)
    d_low = d_scores.astype(jnp.bfloat16)
    d_queries = (
        jnp.einsum("whmn,wnhd->wmhd", d_low, key_vectors, preferred_element_type=jnp.float32)
        * score_scale
    ).astype(jnp.bfloat16)
    d_keys = (
        jnp.einsum("whmn,wmhd->wnhd", d_low, query_rows, preferred_element_type=jnp.float32)
        * score_scale
    ).astype(jnp.bfloat16)
    d_projected = jnp.concatenate(
        [
            d_queries.reshape(total_row_count, inner_width),
            d_keys.reshape(total_row_count, inner_width),
            d_values.reshape(total_row_count, inner_width),
        ],
        axis=1,
    )
    normalized_gradient = lax.dot_general(
        d_projected, qkv_full, (((1,), (1,)), ((), ())), preferred_element_type=jnp.float32
    )
    gain_contribution = jnp.sum(normalized_gradient * standardized_rows, axis=0)
    scaled_rows = normalized_gradient * layer_norm_gain
    branch_gradient = inverse_deviation * (
        scaled_rows
        - jnp.mean(scaled_rows, axis=-1, keepdims=True)
        - standardized_rows * jnp.mean(scaled_rows * standardized_rows, axis=-1, keepdims=True)
    )
    return (branch_gradient.astype(jnp.bfloat16), gain_contribution, table_part)


MESH = pl.DeviceIdType.MESH
VMEM = pltpu.VMEM


def on_device(
    sizes,
    pixels,
    cotangent,
    embed_weight,
    embed_bias,
    layer_norm_gain,
    qkv_weight,
    out_weight,
    bias_table,
    rel_index,
    shifts,
):
    images, rows_dev, cols_dev, features = cotangent.shape
    rows, cols, dps = sizes
    head_count, table_size = bias_table.shape
    pix_block, cot_block = pixels[0], cotangent[0]
    row_shift, col_shift = shifts[0, 0], shifts[0, 1]
    qkv_full, out_full = [
        lax.all_gather(
            lax.all_gather(w, "row", axis=0, tiled=True), ("col", "dp"), axis=1, tiled=True
        )
        for w in (qkv_weight, out_weight)
    ]
    pix_r, cot_r = from_behind((pix_block, cot_block), "row", -1)
    pix_c, cot_c = from_behind((pix_block, cot_block[:, :WIN]), "col", -1)
    pix_x, cot_x = from_behind((pix_c, cot_c), "row", -1)
    wide_pix = jnp.concatenate(
        [
            jnp.concatenate([pix_block, pix_c[:, :, : WIN * PATCH]], axis=2),
            jnp.concatenate([pix_r, pix_x[:, :, : WIN * PATCH]], axis=2),
        ],
        axis=1,
    )
    wide_cot = jnp.concatenate(
        [
            jnp.concatenate([cot_block, cot_c], axis=1),
            jnp.concatenate([cot_r, cot_x], axis=1),
        ],
        axis=0,
    )
    wide_patches = make_patches(wide_pix[None])[0]
    patches = lax.dynamic_slice(
        wide_patches, (row_shift, col_shift, 0), (rows_dev, cols_dev, wide_patches.shape[2])
    )
    shifted_cot = lax.dynamic_slice(
        wide_cot, (row_shift, col_shift, 0), (rows_dev, cols_dev, features)
    )
    patch_rows = window_split(patches).reshape(-1, patches.shape[2])
    cot_flat = window_split(shifted_cot).reshape(-1, features)
    grid_rows, grid_cols = rows_dev * rows, cols_dev * cols
    row_ids = lax.axis_index("row") * rows_dev + jnp.arange(rows_dev, dtype=jnp.int32)
    col_ids = lax.axis_index("col") * cols_dev + jnp.arange(cols_dev, dtype=jnp.int32)
    row_part = (row_ids >= grid_rows - row_shift).astype(jnp.int32)
    col_part = (col_ids >= grid_cols - col_shift).astype(jnp.int32)
    region = 2 * row_part[:, None] + col_part[None, :]
    labels = window_split(region[:, :, None])[:, :, 0]
    selector = (
        rel_index.reshape(-1)[:, None] == jnp.arange(table_size, dtype=jnp.int32)[None, :]
    ).astype(jnp.float32)
    bias_full = jnp.dot(selector, bias_table.T, precision=lax.Precision.HIGHEST).T.reshape(
        head_count, WIN * WIN, WIN * WIN
    )
    cells = embed_cells(patch_rows, embed_weight, embed_bias)
    stored_residuals, attended = attend_forward(
        cells.reshape(-1, WIN * WIN, features), labels, layer_norm_gain, qkv_full, bias_full
    )
    d_attended = lax.dot_general(
        cot_flat, out_full, (((1,), (1,)), ((), ())), preferred_element_type=jnp.float32
    ).astype(jnp.bfloat16)
    d_rows, gain_contribution, table_part = attend_backward(
        stored_residuals, d_attended, layer_norm_gain, qkv_full
    )
    table_grad = jnp.dot(
        table_part.reshape(head_count, -1), selector, precision=lax.Precision.HIGHEST
    )
    contract = (((0,), (0,)), ((), ()))
    back_rows = jnp.concatenate([cot_flat, d_rows], axis=0)
    embed_grad = lax.dot_general(
        jnp.concatenate([patch_rows, patch_rows], axis=0),
        back_rows,
        contract,
        preferred_element_type=jnp.float32,
    )
    bias_grad = jnp.sum(back_rows, axis=0, dtype=jnp.float32)
    partial_rows = lax.psum_scatter(
        lax.dot_general(attended, cot_flat, contract, preferred_element_type=jnp.float32),
        "row",
        scatter_dimension=0,
        tiled=True,
    )
    out_weight_grad = lax.psum_scatter(
        partial_rows, ("col", "dp"), scatter_dimension=1, tiled=True
    )
    totals = lax.psum(
        (embed_grad, bias_grad, gain_contribution, table_grad), ("row", "col", "dp")
    )
    return (out_weight_grad,) + totals


UNROLL = 6


def hand_out(*refs):
    sems = refs[-1]
    count = (len(refs) - 1) // 2
    copies = [
        pltpu.make_async_copy(refs[i], refs[count + i], sems.at[i]) for i in range(count)
    ]
    for copy in copies:
        copy.start()
    for copy in copies:
        copy.wait()


def whole_kernel(
    sizes, heads, patch_width,
    shift_ref, qkv_ref, out_ref, cot_ref, pix_ref, emb_ref, embb_ref, gain_ref, tab_ref, rel_ref,
    grad_out, embed_out, bias_out, gain_out, table_out,
    qkv_all, out_all, cot_o, pat_o, rel_s, bias_t, p_s, cot_c, cot_r, cot_x, pat_c, pat_r, pat_x,
    pat_s, cot_s, xhat_s, inv_s, norm_s, proj_s, datt_s, att_s, dproj_s, bias_s, dtab_s, dn_s,
    gb, core_g, st, a1, b1, t2a, t2b, a2, b2, keep, zs, zr,
    small_s, core_e, es, er, fin,
    send_sem, recv_sem, own_sem, halo_send, halo_recv, red_send, red_recv,
    sml_send, sml_recv, all_send, all_recv, fwd_send, fwd_recv,
):
    bf16, f32, i32 = jnp.bfloat16, jnp.float32, jnp.int32
    rows, cols, dps = sizes
    row, col, dp = lax.axis_index("row"), lax.axis_index("col"), lax.axis_index("dp")
    x, z = row % 2, row // 2
    ring = rows // 2
    top = ring - 1
    core = (col + 1) % 2
    yes = row >= 0
    rows_dev, cols_dev, features = cot_o.shape
    edge = cot_c.shape[1]
    cells = WIN * WIN
    windows = cols_dev // WIN
    inner = att_s.shape[1]
    chip_rows = qkv_all.shape[3]
    groups = qkv_all.shape[0]
    out_width = out_all.shape[3]
    scale = (inner // heads) ** -0.5
    sr, sc = shift_ref[0, 0], shift_ref[0, 1]
    span = 2 * cells
    contract_last = (((1,), (1,)), ((), ()))
    contract_first = (((0,), (0,)), ((), ()))

    over_x = {"row": z * 2 + (x + 1) % 2}
    over_y = {"dp": (dp + 1) % 2}
    over_core = {"col": core}
    above_z = {"row": ((z + 1) % ring) * 2 + x}
    below_z = {"row": ((z + top) % ring) * 2 + x}

    def remote(source, target, send, recv, device):
        return pltpu.make_async_remote_copy(
            src_ref=source, dst_ref=target, send_sem=send, recv_sem=recv,
            device_id=device, device_id_type=MESH,
        )

    def flat(ref):
        return ref[...].reshape(-1, ref.shape[-1])

    barrier = pltpu.get_barrier_semaphore()
    others = 0
    for r in range(rows):
        for c in range(cols):
            for d in range(dps):
                if r or c or d:
                    others += 1
                    pl.semaphore_signal(
                        barrier, inc=1,
                        device_id={"row": (row + r) % rows, "col": (col + c) % cols, "dp": (dp + d) % dps},
                        device_id_type=MESH,
                    )
    local = [
        pltpu.make_async_copy(source, target, own_sem.at[i])
        for i, (source, target) in enumerate(
            (
                (qkv_ref, qkv_all.at[col * 2 + dp, row]),
                (out_ref, out_all.at[col * 2 + dp, row]),
                (cot_ref.at[0], cot_o),
            )
        )
    ]
    for copy in local:
        copy.start()
    pl.semaphore_wait(barrier, others)

    def patchify():
        depth = pat_o.shape[2]
        channels, pixel_rows, pixel_cols = pix_ref.shape[1:]
        pix = pix_ref[0].reshape(channels * pixel_rows, pixel_cols)
        area = PATCH * PATCH
        f = lax.broadcasted_iota(i32, (depth, 1), 0)
        source_row = jnp.where(f < patch_width, (f // area) * pixel_rows + (f % area) // PATCH, -1024)
        row_lane = lax.broadcasted_iota(i32, (depth, channels * pixel_rows), 1)
        column = lax.broadcasted_iota(i32, (depth, pixel_cols), 1) % PATCH
        spot = lax.broadcasted_iota(i32, (cols_dev, pixel_cols), 1) // PATCH
        join = jnp.where(spot == lax.broadcasted_iota(i32, (cols_dev, pixel_cols), 0), 1.0, 0.0).astype(bf16)
        last = lax.broadcasted_iota(i32, (cols_dev, depth), 1) == patch_width
        for i in range(rows_dev):
            choose = jnp.where(row_lane == source_row + i * PATCH, 1.0, 0.0).astype(bf16)
            wide = jnp.dot(choose, pix, preferred_element_type=f32)
            wide = jnp.where(column == f % PATCH, wide, 0.0).astype(bf16)
            cell = lax.dot_general(join, wide, contract_last, preferred_element_type=f32)
            pat_o[i] = jnp.where(last, 1.0, cell).astype(bf16)
        rel_s[...] = jnp.concatenate([rel_ref[...], rel_ref[...]], axis=1)

    started = []
    parts = 2
    step = qkv_all.shape[2] // parts
    last_a = parts

    def slot(a, flag, dy, dx, k):
        which = ((col + flag) % 2) * 2 + (dp + dy) % 2, k * 2 + (x + dx) % 2
        if a == last_a:
            return out_all.at[which]
        return qkv_all.at[which[0], which[1], pl.ds(a * step, step)]

    def mark(a, flag, dy, dx, k):
        return recv_sem.at[a, ((flag * 2 + dy) * 2 + dx) * ring + k]

    def ship(a, dy, dx, k, device, landing, when):
        target = slot(a, 0, dy, dx, k)
        copy = remote(target, target, send_sem.at[len(started)], mark(a, *landing, k), device)
        started.append((copy, when))
        pl.when(when)(copy.start)

    def arrive(a, flag, dy, dx, k, when):
        place = slot(a, flag, dy, dx, k)
        copy = remote(place, place, send_sem.at[0], mark(a, flag, dy, dx, k), over_core)
        pl.when(when)(copy.wait_recv)

    can_up, can_down = z < top, z > 0
    middle = (z == 1) | (z == 2)

    def clamp(k):
        return jnp.minimum(jnp.maximum(k, 0), top)

    def around(j):
        if j == 0:
            return ((z, yes, 0),)
        return ((clamp(z - j), z >= j, 1), (clamp(z + j), z + j <= top, -1))

    def spread_own(a, k, when, way, j):
        if way >= 0 and j < top:
            ship(a, 0, 0, k, above_z, (0, 0, 0), when & can_up)
        if way <= 0 and j < top:
            ship(a, 0, 0, k, below_z, (0, 0, 0), when & can_down)
        ship(a, 0, 0, k, over_y, (0, 1, 0), when)
        ship(a, 0, 0, k, over_x, (0, 0, 1), when)
        ship(a, 0, 0, k, over_core, (1, 0, 0), when)

    def line(a, j):
        for k, when, way in around(j):
            arrive(a, 0, 0, 0, k, when)
            spread_own(a, k, when, way, j)

    def x_line(a, j):
        for k, when, _ in around(j):
            arrive(a, 0, 0, 1, k, when)
            if a == last_a:
                ship(a, 0, 1, k, over_y, (0, 1, 1), when)
            elif j == 0:
                ship(a, 0, 1, k, over_y, (0, 1, 1), when)
            ship(a, 0, 1, k, over_core, (1, 0, 1), when)

    def y_line(a, j):
        for k, when, _ in around(j):
            arrive(a, 0, 1, 0, k, when)
            if a != last_a and j == 1:
                ship(a, 1, 0, k, over_x, (0, 1, 1), when & (k // 2 == z // 2))
            ship(a, 1, 0, k, over_core, (1, 1, 0), when)

    def diagonal(a, j):
        for k, when, _ in around(j):
            arrive(a, 0, 1, 1, k, when)
            if a != last_a and j < 3:
                ship(a, 1, 1, k, above_z, (0, 1, 1), when & middle & (k < 2))
                ship(a, 1, 1, k, below_z, (0, 1, 1), when & middle & (k >= 2))
            ship(a, 1, 1, k, over_core, (1, 1, 1), when)

    def hop(a, h):
        if h == 0:
            spread_own(a, z, yes, 0, 0)
            return
        if h < ring:
            line(a, h)
        if h <= ring:
            x_line(a, h - 1)
        if 2 <= h <= ring + 1:
            diagonal(a, h - 2)
        if h <= ring:
            y_line(a, h - 1)

    def partner(a):
        for dy in range(2):
            for dx in range(2):
                for k in range(ring):
                    arrive(a, 1, dy, dx, k, yes)

    above, left = (row + rows - 1) % rows, (col + cols - 1) % cols
    short = rows_dev - 1
    halos = []

    def halo(source, target, device):
        copy = remote(source, target, halo_send.at[len(halos)], halo_recv.at[len(halos)], device)
        halos.append(copy)
        return copy

    pat_halos = [
        halo(pat_o.at[pl.ds(0, short)], pat_r, {"row": above}),
        halo(pat_o.at[pl.ds(0, short), pl.ds(0, edge)], pat_x, {"row": above, "col": left}),
        halo(pat_o.at[:, pl.ds(0, edge)], pat_c, {"col": left}),
    ]
    cot_side = halo(cot_o.at[:, pl.ds(0, edge)], cot_c, {"col": left})
    cuts = [(r, min(2, short - r)) for r in range(0, short, 2)]
    cot_down = [
        halo(cot_o.at[pl.ds(r, n)], cot_r.at[pl.ds(r, n)], {"row": above}) for r, n in cuts
    ]
    cot_corner = halo(cot_r.at[:, pl.ds(0, edge)], cot_x, {"col": left})

    def picks_of(w):
        m = lax.broadcasted_iota(i32, (cells, 1), 0)
        r = (m // WIN) + sr
        c = w * WIN + (m % WIN) + sc
        up, before = r < rows_dev, c < cols_dev
        picks = []
        for ok, high_of, width_of, r_of, c_of in (
            (up & before, rows_dev, cols_dev, 0, 0),
            (up & ~before, rows_dev, edge, 0, cols_dev),
            (~up & before, short, cols_dev, rows_dev, 0),
            (~up & ~before, short, edge, rows_dev, cols_dev),
        ):
            place = jnp.where(ok, (r - r_of) * width_of + (c - c_of), -1)
            lanes = lax.broadcasted_iota(i32, (cells, high_of * width_of), 1)
            picks.append(jnp.where(lanes == place, 1.0, 0.0).astype(bf16))
        return picks

    def pick(picks, parts):
        got = None
        for one, ref in zip(picks, parts):
            term = jnp.dot(one, flat(ref), preferred_element_type=f32)
            got = term if got is None else got + term
        return got.astype(bf16)

    def prologue(w, carry):
        at = pl.ds(pl.multiple_of(w * cells, cells), cells)
        patch = pick(picks_of(w), (pat_o, pat_c, pat_r, pat_x))
        pat_s[at] = patch
        token = (
            jnp.dot(patch[:, :patch_width], emb_ref[...], preferred_element_type=f32) + embb_ref[...]
        ).astype(bf16).astype(f32)
        mean = jnp.mean(token, axis=-1, keepdims=True)
        centered = token - mean
        inv = lax.rsqrt(jnp.mean(centered * centered, axis=-1, keepdims=True) + norm_epsilon)
        xhat = centered * inv
        xhat_s[at] = xhat
        inv_s[at] = jnp.broadcast_to(inv, (cells, 128))
        norm_s[at] = (xhat * gain_ref[...]).astype(bf16)
        return carry

    def pick_cot(w, carry):
        at = pl.ds(pl.multiple_of(w * cells, cells), cells)
        cot_s[at] = pick(picks_of(w), (cot_o, cot_c, cot_r, cot_x))
        return carry

    def weight_rows(r):
        return jnp.concatenate([qkv_all[g, r] for g in range(groups)], axis=0)

    def project():
        full = jnp.concatenate([weight_rows(r) for r in range(rows)], axis=1)
        for n in range(0, 3 * inner, inner):
            proj_s[:, n : n + inner] = lax.dot_general(
                norm_s[...], full[n : n + inner], contract_last, preferred_element_type=f32
            ).astype(bf16)

    def attended_cot():
        datt = None
        for g in range(groups):
            term = lax.dot_general(
                cot_s[:, g * out_width : (g + 1) * out_width], flat(out_all.at[g]),
                contract_last, preferred_element_type=f32,
            )
            datt = term if datt is None else datt + term
        datt_s[...] = datt.astype(bf16)

    def mask_of(wp):
        m = lax.broadcasted_iota(i32, (span, 1), 0)
        n = lax.broadcasted_iota(i32, (1, 2 * span), 1) % span

        def label(cell):
            win = cell // cells
            r = row * rows_dev + (cell % cells) // WIN
            c = col * cols_dev + (wp * 2 + win) * WIN + cell % WIN
            down = (r >= rows * rows_dev - sr).astype(i32)
            over = (c >= cols * cols_dev - sc).astype(i32)
            return win * 4 + down * 2 + over

        return label(m) == label(n)

    masks = [mask_of(wp) for wp in range(windows // 2)]
    first = lax.broadcasted_iota(i32, (span, span), 1) < cells
    zero = jnp.zeros((span, span), bf16)

    def stacked(value):
        return jnp.concatenate([jnp.where(first, value, zero), jnp.where(first, zero, value)], axis=0)

    def attend(hp, carry):
        at = pl.multiple_of(hp * span, span)
        bias = bias_s[hp]
        bias = jnp.concatenate([bias, bias], axis=0)
        for wp in range(windows // 2):
            rs = slice(wp * span, (wp + 1) * span)
            q = proj_s[rs, pl.ds(at, span)]
            ks = stacked(proj_s[rs, pl.ds(inner + at, span)])
            vs = stacked(proj_s[rs, pl.ds(2 * inner + at, span)])
            s = lax.dot_general(q, ks, contract_last, preferred_element_type=f32)
            s = jnp.where(masks[wp], s * scale + bias, -1e30)
            ps = []
            for half in range(2):
                part = s[:, half * span : (half + 1) * span]
                e = jnp.exp(part - jnp.max(part, axis=-1, keepdims=True))
                ps.append(e * (1.0 / jnp.sum(e, axis=-1, keepdims=True)))
            p = jnp.concatenate(ps, axis=1)
            p_s[hp, wp] = p
            att_s[rs, pl.ds(at, span)] = jnp.dot(
                p.astype(bf16), vs, preferred_element_type=f32
            ).astype(bf16)
        return carry

    def attend_back(hp, carry):
        at = pl.multiple_of(hp * span, span)
        kept = None
        for wp in range(windows // 2):
            rs = slice(wp * span, (wp + 1) * span)
            q = proj_s[rs, pl.ds(at, span)]
            ks = stacked(proj_s[rs, pl.ds(inner + at, span)])
            vs = stacked(proj_s[rs, pl.ds(2 * inner + at, span)])
            do = datt_s[rs, pl.ds(at, span)]
            dprob = lax.dot_general(do, vs, contract_last, preferred_element_type=f32)
            p = p_s[hp, wp]
            dss = []
            for half in range(2):
                part = p[:, half * span : (half + 1) * span]
                d = dprob[:, half * span : (half + 1) * span]
                dss.append(part * (d - jnp.sum(part * d, axis=-1, keepdims=True)))
            p_low = p.astype(bf16)
            ds = jnp.concatenate(dss, axis=1)
            d_low = ds.astype(bf16)
            tab = ds[:cells] + ds[cells:]
            kept = tab if kept is None else kept + tab
            dv = lax.dot_general(p_low, do, contract_first, preferred_element_type=f32)
            dq = jnp.dot(d_low, ks, preferred_element_type=f32) * scale
            dk = lax.dot_general(d_low, q, contract_first, preferred_element_type=f32) * scale
            dproj_s[rs, pl.ds(at, span)] = dq.astype(bf16)
            dproj_s[rs, pl.ds(inner + at, span)] = jnp.where(first, dk[:span], dk[span:]).astype(bf16)
            dproj_s[rs, pl.ds(2 * inner + at, span)] = jnp.where(first, dv[:span], dv[span:]).astype(bf16)
        dtab_s[hp] = kept
        return carry

    def back_project():
        for r in range(0, rows, 2):
            two = jnp.concatenate([weight_rows(r), weight_rows(r + 1)], axis=1)
            dn_s[:, r * chip_rows : (r + 2) * chip_rows] = jnp.dot(
                dproj_s[...], two, preferred_element_type=f32
            )

    def finish(w, gain_sum):
        at = pl.ds(pl.multiple_of(w * cells, cells), cells)
        dn = dn_s[at]
        xhat = xhat_s[at]
        gain_sum = gain_sum + jnp.sum(dn * xhat, axis=0, keepdims=True)
        g_rows = dn * gain_ref[...]
        mean = jnp.mean(g_rows, axis=-1, keepdims=True)
        along = jnp.mean(g_rows * xhat, axis=-1, keepdims=True)
        norm_s[at] = (inv_s[at][:, :1] * (g_rows - mean - xhat * along)).astype(bf16)
        return gain_sum

    entries = lax.broadcasted_iota(i32, (256, 2 * span), 0)

    def spread_of(at):
        pair = jnp.concatenate([rel_s[pl.ds(2 * at, 1), :], rel_s[pl.ds(2 * at + 1, 1), :]], axis=1)
        return jnp.where(entries == pair, 1.0, 0.0).astype(bf16)

    def bias_make(start, stop, final):
        order = [tab_ref[i : i + 1, :] for i in list(range(0, heads, 2)) + list(range(1, heads, 2))]
        rest = jnp.concatenate(order, axis=0)
        rest = jnp.concatenate(
            [rest, jnp.zeros((heads, 256 - rest.shape[1]), f32)], axis=1
        )
        terms = []
        for _ in range(3):
            low = rest.astype(bf16)
            terms.append(low)
            rest = rest - low.astype(f32)
        stack = jnp.concatenate([t.astype(f32) for t in terms], axis=0).astype(bf16)

        def one(i, carry):
            for u in range(4):
                at = i * 4 + u
                got = jnp.dot(stack, spread_of(at), preferred_element_type=f32)
                got = got[:heads] + got[heads : 2 * heads] + got[2 * heads :]
                for v in range(2):
                    piece = got[:, v * span : (v + 1) * span]
                    m = 2 * at + v
                    bias_t[m, : heads // 2, :span] = piece[: heads // 2]
                    bias_t[m, : heads // 2, span:] = piece[heads // 2 :]
            return carry

        lax.fori_loop(start, stop, one, 0)
        for pair in range(heads // 2 if final else 0):
            bias_s[pair] = bias_t[:, pair, :]

    def table_step(i, carry):
        for u in range(4):
            at = i * 4 + u
            one, two = dtab_s[:, at * 2, :], dtab_s[:, at * 2 + 1, :]
            part = jnp.concatenate(
                [
                    jnp.concatenate([one[:, :span], two[:, :span]], axis=1),
                    jnp.concatenate([one[:, span:], two[:, span:]], axis=1),
                ],
                axis=0,
            )
            high = part.astype(bf16).astype(f32)
            both = jnp.concatenate([high, part - high], axis=0).astype(bf16)
            carry = carry + lax.dot_general(
                both, spread_of(at), contract_last, preferred_element_type=f32
            )
        return carry

    pending = []

    def swap(index, source, target, device):
        copy = remote(source, target, red_send.at[index], red_recv.at[index], device)
        copy.start()
        pending.append(copy)
        return copy

    away, over = (x + 1) % 2, (dp + 1) % 2

    def grad_block(g):
        at = pl.ds(pl.multiple_of(g * out_width, out_width), out_width)
        block = lax.dot_general(
            att_s[...], cot_s[:, at], contract_first, preferred_element_type=f32
        )
        gb[g] = block.astype(bf16).reshape(gb.shape[1:])

    def grad_make():
        sent = []
        for i, d in enumerate((over, dp)):
            grad_block(core * 2 + d)
            sent.append(swap(8 + i, gb.at[core * 2 + d], core_g.at[d], over_core))
        for d in (over, dp):
            grad_block(col * 2 + d)
        return sent

    half_rows = st.shape[4]

    def grad_first(got):
        sent = []
        for i, d in enumerate((over, dp)):
            got[i].wait_recv()
            for r in range(rows):
                total = (gb[col * 2 + d, r].astype(f32) + core_g[d, r].astype(f32)).astype(bf16)
                st[0, d, r % 2, r // 2] = total[:half_rows]
                st[1, d, r % 2, r // 2] = total[half_rows:]
            if i == 0:
                sent.append(swap(1, st.at[0, over], a1, over_y))
        sent.append(swap(2, st.at[1, :, away], b1, over_x))
        return sent

    def grad_second(got):
        got[0].wait_recv()
        t2a[...] = (st[0, dp, away].astype(f32) + a1[away].astype(f32)).astype(bf16)
        sent = [swap(3, t2a, a2, over_x)]
        got[1].wait_recv()
        t2b[...] = (st[1, over, x].astype(f32) + b1[over].astype(f32)).astype(bf16)
        sent.append(swap(4, t2b, b2, over_y))
        keep[0] = st[0, dp, x].astype(f32) + a1[x].astype(f32)
        keep[1] = st[1, dp, x].astype(f32) + b1[dp].astype(f32)
        return sent

    def grad_third(got):
        sent = []
        for h, ref in enumerate((a2, b2)):
            got[h].wait_recv()
            keep[h] += ref[...].astype(f32)
            for s in range(1, ring):
                zs[s, h] = keep[h, (z + s) % ring].astype(bf16)
                sent.append(
                    swap(
                        10 + s * 2 + h, zs.at[s, h], zr.at[s, h],
                        {"row": ((z + s) % ring) * 2 + x},
                    )
                )
        return sent

    def grad_last(got):
        for copy in got:
            copy.wait_recv()
        for h in range(2):
            total = keep[h, z]
            for s in range(1, ring):
                total = total + zr[s, h].astype(f32)
            grad_out[h * half_rows : (h + 1) * half_rows] = total

    def unrolled(body):
        def several(i, carry):
            for u in range(UNROLL):
                body(i * UNROLL + u, carry)
            return carry

        lax.fori_loop(0, heads // 2 // UNROLL, several, 0)

    local[0].wait()
    local[1].wait()
    every = parts + 1

    def hops(h):
        for a in range(every):
            hop(a, h)

    hops(0)
    patchify()
    for copy in pat_halos:
        copy.start()
    local[2].wait()
    cot_side.start()
    cot_down[0].start()
    hops(1)
    bias_make(0, cells // 16, False)
    for copy in cot_down[1:-1]:
        copy.start()
    hops(2)
    for copy in pat_halos:
        copy.wait_recv()
    lax.fori_loop(0, windows // 2, prologue, 0)
    cot_down[-1].start()
    hops(3)
    lax.fori_loop(windows // 2, windows, prologue, 0)
    hops(4)
    bias_make(cells // 16, cells // 8, True)
    for copy in cot_down:
        copy.wait_recv()
    cot_corner.start()
    hops(5)
    cot_side.wait_recv()
    cot_corner.wait_recv()
    lax.fori_loop(0, windows, pick_cot, 0)
    for a in range(parts):
        partner(a)
    project()
    unrolled(attend)
    got = grad_make()
    partner(last_a)
    attended_cot()
    got = grad_first(got)
    unrolled(attend_back)
    tab = lax.fori_loop(0, cells // 8, table_step, jnp.zeros((2 * heads, 256), f32))
    tab = tab[:heads] + tab[heads:]
    got = grad_second(got)
    back_project()
    got = grad_third(got)
    gain_sum = lax.fori_loop(0, windows, finish, jnp.zeros((1, features), f32))
    patch = pat_s[...]
    embed = lax.dot_general(patch, cot_s[...], contract_first, preferred_element_type=f32)
    embed = embed + lax.dot_general(patch, norm_s[...], contract_first, preferred_element_type=f32)
    depth = embed.shape[0]
    wide = features // cols
    for c in range(cols):
        for rg in range(depth // 8):
            for lh in range(wide // 256):
                at = c * wide + lh * 256
                small_s[c, rg * (wide // 256) + lh] = embed[rg * 8 : rg * 8 + 8, at : at + 256]
    per = wide // 256
    base = patch_width // 8
    for c in range(cols):
        for lh in range(per):
            at = c * wide + lh * 256
            small_s[c, base * per + lh, 1:2] = gain_sum[:, at : at + 256]
    small_s[0, base * per, 2:8] = tab[: heads // 2]
    small_s[0, (base + 1) * per, 0 : heads // 2] = tab[heads // 2 :]
    flip = remote(small_s.at[core], core_e, sml_send.at[0], sml_recv.at[0], over_core)
    flip.start()
    flip.wait_recv()
    es[...] = small_s[col] + core_e[...]
    spread = []
    for r in range(rows):
        for d in range(dps):
            if r or d:
                to_row, to_dp = (row + r) % rows, (dp + d) % dps
                index = r * dps + d
                copy = remote(
                    es.at[to_row * dps + to_dp], er.at[index], sml_send.at[index], sml_recv.at[index],
                    {"row": to_row, "dp": to_dp},
                )
                copy.start()
                spread.append(copy)
    mine = row * dps + dp
    for copy in spread:
        copy.wait_recv()
    whole = es[mine]
    for index in range(1, rows * dps):
        whole = whole + er[index]
    fin[col, mine] = whole.astype(bf16)
    tell = []
    hand = remote(fin.at[col, mine], fin.at[col, mine], fwd_send.at[0], fwd_recv.at[0], over_core)
    for r in range(rows):
        for d in range(dps):
            if r or d:
                index = r * dps + d
                copy = remote(
                    fin.at[col, mine], fin.at[col, mine], all_send.at[index], all_recv.at[index],
                    {"row": (row + r) % rows, "dp": (dp + d) % dps},
                )
                copy.start()
                tell.append(copy)
    hand.start()
    grad_last(got)
    for r in range(rows):
        for d in range(dps):
            if r or d:
                index = r * dps + d
                part = ((row + rows - r) % rows) * dps + (dp + dps - d) % dps
                place = fin.at[col, part]
                remote(place, place, all_send.at[index], all_recv.at[index], over_core).wait_recv()
                copy = remote(place, place, fwd_send.at[index], fwd_recv.at[index], over_core)
                copy.start()
                tell.append(copy)
    for r in range(rows):
        for d in range(dps):
            index = r * dps + d
            part = ((row + rows - r) % rows) * dps + (dp + dps - d) % dps
            place = fin.at[core, part]
            remote(place, place, fwd_send.at[index], fwd_recv.at[index], over_core).wait_recv()
    for c in range(cols):
        for lh in range(per):
            at = c * wide + lh * 256
            for rg in range(base):
                embed_out[rg * 8 : rg * 8 + 8, at : at + 256] = fin[c, rg * per + lh].astype(f32)
            rest = fin[c, base * per + lh].astype(f32)
            bias_out[:, at : at + 256] = rest[0:1]
            gain_out[:, at : at + 256] = rest[1:2]
    entries_out = table_out.shape[1]
    ones = fin[0, base * per].astype(f32)[:, :entries_out]
    twos = fin[0, (base + 1) * per].astype(f32)[:, :entries_out]
    for i in range(heads // 2):
        table_out[2 * i : 2 * i + 1] = ones[2 + i : 3 + i]
        table_out[2 * i + 1 : 2 * i + 2] = twos[i : i + 1]
    for copy, when in started:
        pl.when(when)(copy.wait_send)
    for copy in halos + pending + [flip] + spread + tell + [hand]:
        copy.wait_send()


def direct_device(
    sizes, pixels, cotangent, embed_weight, embed_bias, layer_norm_gain,
    qkv_weight, out_weight, bias_table, rel_index, shifts,
):
    rows, cols, dps = sizes
    ring = rows // 2
    heads, table_size = bias_table.shape
    patch_width, features = embed_weight.shape
    bf16, f32 = jnp.bfloat16, jnp.float32
    _, rows_dev, cols_dev, _ = cotangent.shape
    groups = cols * dps
    depth = 64
    cells = WIN * WIN
    inner = out_weight.shape[0] * rows
    here = rows_dev * cols_dev
    big = out_weight.shape
    half = big[0] // 2
    dma = pltpu.SemaphoreType.DMA
    vmem = pl.BlockSpec(memory_space=VMEM)
    sums = (rows * dps, 8, 256)
    grad, embed, bias, gain, table = pl.pallas_call(
        functools.partial(whole_kernel, sizes, heads, patch_width),
        out_shape=[
            jax.ShapeDtypeStruct(big, f32),
            jax.ShapeDtypeStruct((patch_width, features), f32),
            jax.ShapeDtypeStruct((1, features), f32),
            jax.ShapeDtypeStruct((1, features), f32),
            jax.ShapeDtypeStruct((heads, table_size), f32),
        ],
        in_specs=[pl.BlockSpec(memory_space=pltpu.SMEM)] + [pl.BlockSpec(memory_space=pl.ANY)] * 3 + [vmem] * 6,
        out_specs=[vmem] * 5,
        scratch_shapes=[
            VMEM((groups, rows) + qkv_weight.shape[::-1], bf16),
            VMEM((groups, rows) + big, bf16),
            VMEM((rows_dev, cols_dev, features), bf16),
            VMEM((rows_dev, cols_dev, depth), bf16),
            VMEM((cells, 2 * cells), jnp.int32),
            VMEM((cells, 8 * pl.cdiv(heads, 16), 4 * cells), f32),
            VMEM((heads // 2, cols_dev // (2 * WIN), 2 * cells, 4 * cells), f32),
            VMEM((rows_dev, WIN, features), bf16),
            VMEM((rows_dev - 1, cols_dev, features), bf16),
            VMEM((rows_dev - 1, WIN, features), bf16),
            VMEM((rows_dev, WIN, depth), bf16),
            VMEM((rows_dev - 1, cols_dev, depth), bf16),
            VMEM((rows_dev - 1, WIN, depth), bf16),
            VMEM((here, depth), bf16),
            VMEM((here, features), bf16),
            VMEM((here, features), f32),
            VMEM((here, 128), f32),
            VMEM((here, features), bf16),
            VMEM((here, 3 * inner), bf16),
            VMEM((here, inner), bf16),
            VMEM((here, inner), bf16),
            VMEM((here, 3 * inner), bf16),
            VMEM((heads // 2, cells, 4 * cells), f32),
            VMEM((heads // 2, cells, 4 * cells), f32),
            VMEM((here, features), f32),
            VMEM((groups, rows) + big, bf16),
            VMEM((2, rows) + big, bf16),
            VMEM((2, 2, 2, ring, half, big[1]), bf16),
            VMEM((2, ring, half, big[1]), bf16),
            VMEM((2, ring, half, big[1]), bf16),
            VMEM((ring, half, big[1]), bf16),
            VMEM((ring, half, big[1]), bf16),
            VMEM((ring, half, big[1]), bf16),
            VMEM((ring, half, big[1]), bf16),
            VMEM((2, ring, half, big[1]), f32),
            VMEM((ring, 2, half, big[1]), bf16),
            VMEM((ring, 2, half, big[1]), bf16),
            VMEM((cols,) + sums, f32),
            VMEM(sums, f32), VMEM(sums, f32), VMEM(sums, f32),
            VMEM((cols,) + sums, bf16),
            dma((400,)), dma((3, 8 * ring)), dma((3,)), dma((16,)), dma((16,)),
            dma((20,)), dma((20,)),
            dma((rows * dps,)), dma((rows * dps,)), dma((rows * dps,)), dma((rows * dps,)),
            dma((rows * dps,)), dma((rows * dps,)),
        ],
        compiler_params=pltpu.CompilerParams(
            collective_id=0, has_side_effects=True, vmem_limit_bytes=60 * 2**20
        ),
        name="whole",
    )(
        shifts, qkv_weight.T, out_weight, cotangent, pixels, embed_weight,
        embed_bias[None], layer_norm_gain[None], bias_table, rel_index,
    )
    results = (grad, embed, bias, gain, table)
    grad, embed, bias, gain, table = pl.pallas_call(
        hand_out,
        out_shape=[jax.ShapeDtypeStruct(value.shape, value.dtype) for value in results],
        in_specs=[vmem] * 5,
        out_specs=[pl.BlockSpec(memory_space=pl.ANY)] * 5,
        scratch_shapes=[dma((5,))],
        name="hand_out",
    )(*results)
    return (grad, embed, bias[0], gain[0], table)


def solution(mesh):
    sizes = tuple(mesh.shape[name] for name in ("row", "col", "dp"))
    direct = sizes[1:] == (2, 2) and sizes[0] == 8
    return jax.shard_map(
        functools.partial(direct_device if direct else on_device, sizes),
        mesh=mesh,
        in_specs=(
            P("dp", None, "row", "col"),
            P("dp", "row", "col", None),
            P(),
            P(),
            P(),
            P("row", ("col", "dp")),
            P("row", ("col", "dp")),
            P(),
            P(),
            P("dp", None),
        ),
        out_specs=(P("row", ("col", "dp")), P(), P(), P(), P()),
        check_vma=False,
    )
```

```python
import functools

import jax
import jax.numpy as jnp
from jax import lax
from jax.experimental import pallas as pl
from jax.experimental.pallas import tpu as pltpu
from jax.sharding import PartitionSpec as P

WIN = 8
PATCH = 4


norm_epsilon = 1e-05


def from_behind(value, axis, steps):
    count = lax.axis_size(axis)
    pairs = [(source, (source + steps) % count) for source in range(count)]
    return lax.ppermute(value, axis, pairs)


def make_patches(pixel_block):
    images, channels, pixel_rows, pixel_cols = pixel_block.shape
    grid_rows = pixel_rows // PATCH
    grid_cols = pixel_cols // PATCH
    shaped = pixel_block.reshape(images, channels, grid_rows, PATCH, grid_cols, PATCH)
    return shaped.transpose(0, 2, 4, 1, 3, 5).reshape(
        images, grid_rows, grid_cols, channels * PATCH * PATCH
    )


def embed_cells(patches, embed_weight, embed_bias):
    return (jnp.dot(patches, embed_weight, preferred_element_type=jnp.float32) + embed_bias).astype(
        jnp.bfloat16
    )


def window_split(block):
    rows_all, cols_all, features = block.shape
    shaped = block.reshape(rows_all // WIN, WIN, cols_all // WIN, WIN, features)
    return shaped.transpose(0, 2, 1, 3, 4).reshape(-1, WIN * WIN, features)


def window_join(windows, rows_all, cols_all):
    features = windows.shape[-1]
    shaped = windows.reshape(rows_all // WIN, cols_all // WIN, WIN, WIN, features)
    return shaped.transpose(0, 2, 1, 3, 4).reshape(rows_all, cols_all, features)

def attend_forward(cell_windows, labels, layer_norm_gain, qkv_full, bias_full):
    window_count, cell_count, features = cell_windows.shape
    head_count = bias_full.shape[0]
    inner_width = qkv_full.shape[1] // 3
    head_size = inner_width // head_count
    score_scale = head_size ** (-0.5)
    flat_rows = cell_windows.reshape(-1, features).astype(jnp.float32)
    average = jnp.mean(flat_rows, axis=-1, keepdims=True)
    centered_input = flat_rows - average
    inverse_deviation = lax.rsqrt(
        jnp.mean(centered_input * centered_input, axis=-1, keepdims=True) + norm_epsilon
    )
    standardized_rows = centered_input * inverse_deviation
    normalized_rows = (standardized_rows * layer_norm_gain).astype(jnp.bfloat16)
    projected = jnp.dot(normalized_rows, qkv_full, preferred_element_type=jnp.float32).astype(
        jnp.bfloat16
    )
    head_shape = (window_count, cell_count, head_count, head_size)
    query_rows = projected[:, :inner_width].reshape(head_shape)
    key_vectors = projected[:, inner_width : 2 * inner_width].reshape(head_shape)
    value_rows = projected[:, 2 * inner_width :].reshape(head_shape)
    scores = (
        jnp.einsum("wmhd,wnhd->whmn", query_rows, key_vectors, preferred_element_type=jnp.float32)
        * score_scale
        + bias_full[None]
    )
    same_region = labels[:, None, :, None] == labels[:, None, None, :]
    scores = jnp.where(same_region, scores, -1e30)
    row_peak = jnp.max(scores, axis=-1, keepdims=True)
    exp_scores = jnp.exp(scores - row_peak)
    attention_weights = exp_scores / jnp.sum(exp_scores, axis=-1, keepdims=True)
    reduced_probability = attention_weights.astype(jnp.bfloat16)
    attended = jnp.einsum(
        "whmn,wnhd->wmhd", reduced_probability, value_rows, preferred_element_type=jnp.float32
    ).astype(jnp.bfloat16)
    stored_residuals = (
        standardized_rows,
        inverse_deviation,
        query_rows,
        key_vectors,
        value_rows,
        attention_weights,
        reduced_probability,
    )
    return (stored_residuals, attended.reshape(-1, inner_width))


def attend_backward(stored_residuals, d_attended, layer_norm_gain, qkv_full):
    (
        standardized_rows,
        inverse_deviation,
        query_rows,
        key_vectors,
        value_rows,
        attention_weights,
        reduced_probability,
    ) = stored_residuals
    head_shape = query_rows.shape
    score_scale = head_shape[3] ** (-0.5)
    total_row_count = standardized_rows.shape[0]
    inner_width = head_shape[2] * head_shape[3]
    d_heads = d_attended.reshape(head_shape)
    d_prob = jnp.einsum("wmhd,wnhd->whmn", d_heads, value_rows, preferred_element_type=jnp.float32)
    d_values = jnp.einsum(
        "whmn,wmhd->wnhd", reduced_probability, d_heads, preferred_element_type=jnp.float32
    ).astype(jnp.bfloat16)
    d_scores = attention_weights * (
        d_prob - jnp.sum(attention_weights * d_prob, axis=-1, keepdims=True)
    )
    table_part = jnp.sum(d_scores, axis=0)
    d_low = d_scores.astype(jnp.bfloat16)
    d_queries = (
        jnp.einsum("whmn,wnhd->wmhd", d_low, key_vectors, preferred_element_type=jnp.float32)
        * score_scale
    ).astype(jnp.bfloat16)
    d_keys = (
        jnp.einsum("whmn,wmhd->wnhd", d_low, query_rows, preferred_element_type=jnp.float32)
        * score_scale
    ).astype(jnp.bfloat16)
    d_projected = jnp.concatenate(
        [
            d_queries.reshape(total_row_count, inner_width),
            d_keys.reshape(total_row_count, inner_width),
            d_values.reshape(total_row_count, inner_width),
        ],
        axis=1,
    )
    normalized_gradient = lax.dot_general(
        d_projected, qkv_full, (((1,), (1,)), ((), ())), preferred_element_type=jnp.float32
    )
    gain_contribution = jnp.sum(normalized_gradient * standardized_rows, axis=0)
    scaled_rows = normalized_gradient * layer_norm_gain
    branch_gradient = inverse_deviation * (
        scaled_rows
        - jnp.mean(scaled_rows, axis=-1, keepdims=True)
        - standardized_rows * jnp.mean(scaled_rows * standardized_rows, axis=-1, keepdims=True)
    )
    return (branch_gradient.astype(jnp.bfloat16), gain_contribution, table_part)


MESH = pl.DeviceIdType.MESH
VMEM = pltpu.VMEM


def on_device(
    sizes,
    pixels,
    cotangent,
    embed_weight,
    embed_bias,
    layer_norm_gain,
    qkv_weight,
    out_weight,
    bias_table,
    rel_index,
    shifts,
):
    images, rows_dev, cols_dev, features = cotangent.shape
    rows, cols, dps = sizes
    head_count, table_size = bias_table.shape
    pix_block, cot_block = pixels[0], cotangent[0]
    row_shift, col_shift = shifts[0, 0], shifts[0, 1]
    qkv_full, out_full = [
        lax.all_gather(
            lax.all_gather(w, "row", axis=0, tiled=True), ("col", "dp"), axis=1, tiled=True
        )
        for w in (qkv_weight, out_weight)
    ]
    pix_r, cot_r = from_behind((pix_block, cot_block), "row", -1)
    pix_c, cot_c = from_behind((pix_block, cot_block[:, :WIN]), "col", -1)
    pix_x, cot_x = from_behind((pix_c, cot_c), "row", -1)
    wide_pix = jnp.concatenate(
        [
            jnp.concatenate([pix_block, pix_c[:, :, : WIN * PATCH]], axis=2),
            jnp.concatenate([pix_r, pix_x[:, :, : WIN * PATCH]], axis=2),
        ],
        axis=1,
    )
    wide_cot = jnp.concatenate(
        [
            jnp.concatenate([cot_block, cot_c], axis=1),
            jnp.concatenate([cot_r, cot_x], axis=1),
        ],
        axis=0,
    )
    wide_patches = make_patches(wide_pix[None])[0]
    patches = lax.dynamic_slice(
        wide_patches, (row_shift, col_shift, 0), (rows_dev, cols_dev, wide_patches.shape[2])
    )
    shifted_cot = lax.dynamic_slice(
        wide_cot, (row_shift, col_shift, 0), (rows_dev, cols_dev, features)
    )
    patch_rows = window_split(patches).reshape(-1, patches.shape[2])
    cot_flat = window_split(shifted_cot).reshape(-1, features)
    grid_rows, grid_cols = rows_dev * rows, cols_dev * cols
    row_ids = lax.axis_index("row") * rows_dev + jnp.arange(rows_dev, dtype=jnp.int32)
    col_ids = lax.axis_index("col") * cols_dev + jnp.arange(cols_dev, dtype=jnp.int32)
    row_part = (row_ids >= grid_rows - row_shift).astype(jnp.int32)
    col_part = (col_ids >= grid_cols - col_shift).astype(jnp.int32)
    region = 2 * row_part[:, None] + col_part[None, :]
    labels = window_split(region[:, :, None])[:, :, 0]
    selector = (
        rel_index.reshape(-1)[:, None] == jnp.arange(table_size, dtype=jnp.int32)[None, :]
    ).astype(jnp.float32)
    bias_full = jnp.dot(selector, bias_table.T, precision=lax.Precision.HIGHEST).T.reshape(
        head_count, WIN * WIN, WIN * WIN
    )
    cells = embed_cells(patch_rows, embed_weight, embed_bias)
    stored_residuals, attended = attend_forward(
        cells.reshape(-1, WIN * WIN, features), labels, layer_norm_gain, qkv_full, bias_full
    )
    d_attended = lax.dot_general(
        cot_flat, out_full, (((1,), (1,)), ((), ())), preferred_element_type=jnp.float32
    ).astype(jnp.bfloat16)
    d_rows, gain_contribution, table_part = attend_backward(
        stored_residuals, d_attended, layer_norm_gain, qkv_full
    )
    table_grad = jnp.dot(
        table_part.reshape(head_count, -1), selector, precision=lax.Precision.HIGHEST
    )
    contract = (((0,), (0,)), ((), ()))
    back_rows = jnp.concatenate([cot_flat, d_rows], axis=0)
    embed_grad = lax.dot_general(
        jnp.concatenate([patch_rows, patch_rows], axis=0),
        back_rows,
        contract,
        preferred_element_type=jnp.float32,
    )
    bias_grad = jnp.sum(back_rows, axis=0, dtype=jnp.float32)
    partial_rows = lax.psum_scatter(
        lax.dot_general(attended, cot_flat, contract, preferred_element_type=jnp.float32),
        "row",
        scatter_dimension=0,
        tiled=True,
    )
    out_weight_grad = lax.psum_scatter(
        partial_rows, ("col", "dp"), scatter_dimension=1, tiled=True
    )
    totals = lax.psum(
        (embed_grad, bias_grad, gain_contribution, table_grad), ("row", "col", "dp")
    )
    return (out_weight_grad,) + totals


UNROLL = 6


def hand_out(*refs):
    sems = refs[-1]
    count = (len(refs) - 1) // 2
    copies = [
        pltpu.make_async_copy(refs[i], refs[count + i], sems.at[i]) for i in range(count)
    ]
    for copy in copies:
        copy.start()
    for copy in copies:
        copy.wait()


def whole_kernel(
    sizes, heads, patch_width,
    shift_ref, qkv_ref, out_ref, cot_ref, pix_ref, emb_ref, embb_ref, gain_ref, tab_ref, rel_ref,
    grad_out, embed_out, bias_out, gain_out, table_out,
    qkv_all, out_all, cot_o, pat_o, rel_s, bias_t, p_s, cot_c, cot_r, cot_x, pat_c, pat_r, pat_x,
    pat_s, cot_s, xhat_s, inv_s, norm_s, proj_s, datt_s, att_s, dproj_s, bias_s, dtab_s, dn_s,
    gb, core_g, st, a1, b1, t2a, t2b, a2, b2, keep, zs, zr,
    small_s, core_e, es, er, fin,
    send_sem, recv_sem, own_sem, halo_send, halo_recv, red_send, red_recv,
    sml_send, sml_recv, all_send, all_recv, fwd_send, fwd_recv,
):
    bf16, f32, i32 = jnp.bfloat16, jnp.float32, jnp.int32
    rows, cols, dps = sizes
    row, col, dp = lax.axis_index("row"), lax.axis_index("col"), lax.axis_index("dp")
    x, z = row % 2, row // 2
    ring = rows // 2
    top = ring - 1
    core = (col + 1) % 2
    yes = row >= 0
    rows_dev, cols_dev, features = cot_o.shape
    edge = cot_c.shape[1]
    cells = WIN * WIN
    windows = cols_dev // WIN
    inner = att_s.shape[1]
    chip_rows = qkv_all.shape[3]
    groups = qkv_all.shape[0]
    out_width = out_all.shape[3]
    scale = (inner // heads) ** -0.5
    sr, sc = shift_ref[0, 0], shift_ref[0, 1]
    span = 2 * cells
    contract_last = (((1,), (1,)), ((), ()))
    contract_first = (((0,), (0,)), ((), ()))

    over_x = {"row": z * 2 + (x + 1) % 2}
    over_y = {"dp": (dp + 1) % 2}
    over_core = {"col": core}
    above_z = {"row": ((z + 1) % ring) * 2 + x}
    below_z = {"row": ((z + top) % ring) * 2 + x}

    def remote(source, target, send, recv, device):
        return pltpu.make_async_remote_copy(
            src_ref=source, dst_ref=target, send_sem=send, recv_sem=recv,
            device_id=device, device_id_type=MESH,
        )

    def flat(ref):
        return ref[...].reshape(-1, ref.shape[-1])

    barrier = pltpu.get_barrier_semaphore()
    others = 0
    for r in range(rows):
        for c in range(cols):
            for d in range(dps):
                if r or c or d:
                    others += 1
                    pl.semaphore_signal(
                        barrier, inc=1,
                        device_id={"row": (row + r) % rows, "col": (col + c) % cols, "dp": (dp + d) % dps},
                        device_id_type=MESH,
                    )
    local = [
        pltpu.make_async_copy(source, target, own_sem.at[i])
        for i, (source, target) in enumerate(
            (
                (qkv_ref, qkv_all.at[col * 2 + dp, row]),
                (out_ref, out_all.at[col * 2 + dp, row]),
                (cot_ref.at[0], cot_o),
            )
        )
    ]
    for copy in local:
        copy.start()
    pl.semaphore_wait(barrier, others)

    def patchify():
        depth = pat_o.shape[2]
        channels, pixel_rows, pixel_cols = pix_ref.shape[1:]
        pix = pix_ref[0].reshape(channels * pixel_rows, pixel_cols)
        area = PATCH * PATCH
        f = lax.broadcasted_iota(i32, (depth, 1), 0)
        source_row = jnp.where(f < patch_width, (f // area) * pixel_rows + (f % area) // PATCH, -1024)
        row_lane = lax.broadcasted_iota(i32, (depth, channels * pixel_rows), 1)
        column = lax.broadcasted_iota(i32, (depth, pixel_cols), 1) % PATCH
        spot = lax.broadcasted_iota(i32, (cols_dev, pixel_cols), 1) // PATCH
        join = jnp.where(spot == lax.broadcasted_iota(i32, (cols_dev, pixel_cols), 0), 1.0, 0.0).astype(bf16)
        last = lax.broadcasted_iota(i32, (cols_dev, depth), 1) == patch_width
        for i in range(rows_dev):
            choose = jnp.where(row_lane == source_row + i * PATCH, 1.0, 0.0).astype(bf16)
            wide = jnp.dot(choose, pix, preferred_element_type=f32)
            wide = jnp.where(column == f % PATCH, wide, 0.0).astype(bf16)
            cell = lax.dot_general(join, wide, contract_last, preferred_element_type=f32)
            pat_o[i] = jnp.where(last, 1.0, cell).astype(bf16)
        rel_s[...] = jnp.concatenate([rel_ref[...], rel_ref[...]], axis=1)

    started = []
    parts = 2
    step = qkv_all.shape[2] // parts
    last_a = parts

    def slot(a, flag, dy, dx, k):
        which = ((col + flag) % 2) * 2 + (dp + dy) % 2, k * 2 + (x + dx) % 2
        if a == last_a:
            return out_all.at[which]
        return qkv_all.at[which[0], which[1], pl.ds(a * step, step)]

    def mark(a, flag, dy, dx, k):
        return recv_sem.at[a, ((flag * 2 + dy) * 2 + dx) * ring + k]

    def ship(a, dy, dx, k, device, landing, when):
        target = slot(a, 0, dy, dx, k)
        copy = remote(target, target, send_sem.at[len(started)], mark(a, *landing, k), device)
        started.append((copy, when))
        pl.when(when)(copy.start)

    def arrive(a, flag, dy, dx, k, when):
        place = slot(a, flag, dy, dx, k)
        copy = remote(place, place, send_sem.at[0], mark(a, flag, dy, dx, k), over_core)
        pl.when(when)(copy.wait_recv)

    can_up, can_down = z < top, z > 0
    middle = (z == 1) | (z == 2)

    def clamp(k):
        return jnp.minimum(jnp.maximum(k, 0), top)

    def around(j):
        if j == 0:
            return ((z, yes, 0),)
        return ((clamp(z - j), z >= j, 1), (clamp(z + j), z + j <= top, -1))

    def spread_own(a, k, when, way, j):
        if way >= 0 and j < top:
            ship(a, 0, 0, k, above_z, (0, 0, 0), when & can_up)
        if way <= 0 and j < top:
            ship(a, 0, 0, k, below_z, (0, 0, 0), when & can_down)
        ship(a, 0, 0, k, over_y, (0, 1, 0), when)
        ship(a, 0, 0, k, over_x, (0, 0, 1), when)
        ship(a, 0, 0, k, over_core, (1, 0, 0), when)

    def line(a, j):
        for k, when, way in around(j):
            arrive(a, 0, 0, 0, k, when)
            spread_own(a, k, when, way, j)

    def x_line(a, j):
        for k, when, _ in around(j):
            arrive(a, 0, 0, 1, k, when)
            if a == last_a:
                ship(a, 0, 1, k, over_y, (0, 1, 1), when)
            elif j == 0:
                ship(a, 0, 1, k, over_y, (0, 1, 1), when)
            ship(a, 0, 1, k, over_core, (1, 0, 1), when)

    def y_line(a, j):
        for k, when, _ in around(j):
            arrive(a, 0, 1, 0, k, when)
            if a != last_a and j == 1:
                ship(a, 1, 0, k, over_x, (0, 1, 1), when & (k // 2 == z // 2))
            ship(a, 1, 0, k, over_core, (1, 1, 0), when)

    def diagonal(a, j):
        for k, when, _ in around(j):
            arrive(a, 0, 1, 1, k, when)
            if a != last_a and j < 3:
                ship(a, 1, 1, k, above_z, (0, 1, 1), when & middle & (k < 2))
                ship(a, 1, 1, k, below_z, (0, 1, 1), when & middle & (k >= 2))
            ship(a, 1, 1, k, over_core, (1, 1, 1), when)

    def hop(a, h):
        if h == 0:
            spread_own(a, z, yes, 0, 0)
            return
        if h < ring:
            line(a, h)
        if h <= ring:
            x_line(a, h - 1)
        if 2 <= h <= ring + 1:
            diagonal(a, h - 2)
        if h <= ring:
            y_line(a, h - 1)

    def partner(a):
        for dy in range(2):
            for dx in range(2):
                for k in range(ring):
                    arrive(a, 1, dy, dx, k, yes)

    above, left = (row + rows - 1) % rows, (col + cols - 1) % cols
    short = rows_dev - 1
    halos = []

    def halo(source, target, device):
        copy = remote(source, target, halo_send.at[len(halos)], halo_recv.at[len(halos)], device)
        halos.append(copy)
        return copy

    pat_halos = [
        halo(pat_o.at[pl.ds(0, short)], pat_r, {"row": above}),
        halo(pat_o.at[pl.ds(0, short), pl.ds(0, edge)], pat_x, {"row": above, "col": left}),
        halo(pat_o.at[:, pl.ds(0, edge)], pat_c, {"col": left}),
    ]
    cot_side = halo(cot_o.at[:, pl.ds(0, edge)], cot_c, {"col": left})
    cuts = [(r, min(2, short - r)) for r in range(0, short, 2)]
    cot_down = [
        halo(cot_o.at[pl.ds(r, n)], cot_r.at[pl.ds(r, n)], {"row": above}) for r, n in cuts
    ]
    cot_corner = halo(cot_r.at[:, pl.ds(0, edge)], cot_x, {"col": left})

    def picks_of(w):
        m = lax.broadcasted_iota(i32, (cells, 1), 0)
        r = (m // WIN) + sr
        c = w * WIN + (m % WIN) + sc
        up, before = r < rows_dev, c < cols_dev
        picks = []
        for ok, high_of, width_of, r_of, c_of in (
            (up & before, rows_dev, cols_dev, 0, 0),
            (up & ~before, rows_dev, edge, 0, cols_dev),
            (~up & before, short, cols_dev, rows_dev, 0),
            (~up & ~before, short, edge, rows_dev, cols_dev),
        ):
            place = jnp.where(ok, (r - r_of) * width_of + (c - c_of), -1)
            lanes = lax.broadcasted_iota(i32, (cells, high_of * width_of), 1)
            picks.append(jnp.where(lanes == place, 1.0, 0.0).astype(bf16))
        return picks

    def pick(picks, parts):
        got = None
        for one, ref in zip(picks, parts):
            term = jnp.dot(one, flat(ref), preferred_element_type=f32)
            got = term if got is None else got + term
        return got.astype(bf16)

    def prologue(w, carry):
        at = pl.ds(pl.multiple_of(w * cells, cells), cells)
        patch = pick(picks_of(w), (pat_o, pat_c, pat_r, pat_x))
        pat_s[at] = patch
        token = (
            jnp.dot(patch[:, :patch_width], emb_ref[...], preferred_element_type=f32) + embb_ref[...]
        ).astype(bf16).astype(f32)
        mean = jnp.mean(token, axis=-1, keepdims=True)
        centered = token - mean
        inv = lax.rsqrt(jnp.mean(centered * centered, axis=-1, keepdims=True) + norm_epsilon)
        xhat = centered * inv
        xhat_s[at] = xhat
        inv_s[at] = jnp.broadcast_to(inv, (cells, 128))
        norm_s[at] = (xhat * gain_ref[...]).astype(bf16)
        return carry

    def pick_cot(w, carry):
        at = pl.ds(pl.multiple_of(w * cells, cells), cells)
        cot_s[at] = pick(picks_of(w), (cot_o, cot_c, cot_r, cot_x))
        return carry

    def weight_rows(r):
        return jnp.concatenate([qkv_all[g, r] for g in range(groups)], axis=0)

    def project():
        full = jnp.concatenate([weight_rows(r) for r in range(rows)], axis=1)
        for n in range(0, 3 * inner, inner):
            proj_s[:, n : n + inner] = lax.dot_general(
                norm_s[...], full[n : n + inner], contract_last, preferred_element_type=f32
            ).astype(bf16)

    def attended_cot():
        datt = None
        for g in range(groups):
            term = lax.dot_general(
                cot_s[:, g * out_width : (g + 1) * out_width], flat(out_all.at[g]),
                contract_last, preferred_element_type=f32,
            )
            datt = term if datt is None else datt + term
        datt_s[...] = datt.astype(bf16)

    def mask_of(wp):
        m = lax.broadcasted_iota(i32, (span, 1), 0)
        n = lax.broadcasted_iota(i32, (1, 2 * span), 1) % span

        def label(cell):
            win = cell // cells
            r = row * rows_dev + (cell % cells) // WIN
            c = col * cols_dev + (wp * 2 + win) * WIN + cell % WIN
            down = (r >= rows * rows_dev - sr).astype(i32)
            over = (c >= cols * cols_dev - sc).astype(i32)
            return win * 4 + down * 2 + over

        return label(m) == label(n)

    masks = [mask_of(wp) for wp in range(windows // 2)]
    first = lax.broadcasted_iota(i32, (span, span), 1) < cells
    zero = jnp.zeros((span, span), bf16)

    def stacked(value):
        return jnp.concatenate([jnp.where(first, value, zero), jnp.where(first, zero, value)], axis=0)

    def attend(hp, carry):
        at = pl.multiple_of(hp * span, span)
        bias = bias_s[hp]
        bias = jnp.concatenate([bias, bias], axis=0)
        for wp in range(windows // 2):
            rs = slice(wp * span, (wp + 1) * span)
            q = proj_s[rs, pl.ds(at, span)]
            ks = stacked(proj_s[rs, pl.ds(inner + at, span)])
            vs = stacked(proj_s[rs, pl.ds(2 * inner + at, span)])
            s = lax.dot_general(q, ks, contract_last, preferred_element_type=f32)
            s = jnp.where(masks[wp], s * scale + bias, -1e30)
            ps = []
            for half in range(2):
                part = s[:, half * span : (half + 1) * span]
                e = jnp.exp(part - jnp.max(part, axis=-1, keepdims=True))
                ps.append(e * (1.0 / jnp.sum(e, axis=-1, keepdims=True)))
            p = jnp.concatenate(ps, axis=1)
            p_s[hp, wp] = p
            att_s[rs, pl.ds(at, span)] = jnp.dot(
                p.astype(bf16), vs, preferred_element_type=f32
            ).astype(bf16)
        return carry

    def attend_back(hp, carry):
        at = pl.multiple_of(hp * span, span)
        kept = None
        for wp in range(windows // 2):
            rs = slice(wp * span, (wp + 1) * span)
            q = proj_s[rs, pl.ds(at, span)]
            ks = stacked(proj_s[rs, pl.ds(inner + at, span)])
            vs = stacked(proj_s[rs, pl.ds(2 * inner + at, span)])
            do = datt_s[rs, pl.ds(at, span)]
            dprob = lax.dot_general(do, vs, contract_last, preferred_element_type=f32)
            p = p_s[hp, wp]
            dss = []
            for half in range(2):
                part = p[:, half * span : (half + 1) * span]
                d = dprob[:, half * span : (half + 1) * span]
                dss.append(part * (d - jnp.sum(part * d, axis=-1, keepdims=True)))
            p_low = p.astype(bf16)
            ds = jnp.concatenate(dss, axis=1)
            d_low = ds.astype(bf16)
            tab = ds[:cells] + ds[cells:]
            kept = tab if kept is None else kept + tab
            dv = lax.dot_general(p_low, do, contract_first, preferred_element_type=f32)
            dq = jnp.dot(d_low, ks, preferred_element_type=f32) * scale
            dk = lax.dot_general(d_low, q, contract_first, preferred_element_type=f32) * scale
            dproj_s[rs, pl.ds(at, span)] = dq.astype(bf16)
            dproj_s[rs, pl.ds(inner + at, span)] = jnp.where(first, dk[:span], dk[span:]).astype(bf16)
            dproj_s[rs, pl.ds(2 * inner + at, span)] = jnp.where(first, dv[:span], dv[span:]).astype(bf16)
        dtab_s[hp] = kept
        return carry

    def back_project():
        for r in range(0, rows, 2):
            two = jnp.concatenate([weight_rows(r), weight_rows(r + 1)], axis=1)
            dn_s[:, r * chip_rows : (r + 2) * chip_rows] = jnp.dot(
                dproj_s[...], two, preferred_element_type=f32
            )

    def finish(w, gain_sum):
        at = pl.ds(pl.multiple_of(w * cells, cells), cells)
        dn = dn_s[at]
        xhat = xhat_s[at]
        gain_sum = gain_sum + jnp.sum(dn * xhat, axis=0, keepdims=True)
        g_rows = dn * gain_ref[...]
        mean = jnp.mean(g_rows, axis=-1, keepdims=True)
        along = jnp.mean(g_rows * xhat, axis=-1, keepdims=True)
        norm_s[at] = (inv_s[at][:, :1] * (g_rows - mean - xhat * along)).astype(bf16)
        return gain_sum

    entries = lax.broadcasted_iota(i32, (256, 2 * span), 0)

    def spread_of(at):
        pair = jnp.concatenate([rel_s[pl.ds(2 * at, 1), :], rel_s[pl.ds(2 * at + 1, 1), :]], axis=1)
        return jnp.where(entries == pair, 1.0, 0.0).astype(bf16)

    def bias_make(start, stop, final):
        order = [tab_ref[i : i + 1, :] for i in list(range(0, heads, 2)) + list(range(1, heads, 2))]
        rest = jnp.concatenate(order, axis=0)
        rest = jnp.concatenate(
            [rest, jnp.zeros((heads, 256 - rest.shape[1]), f32)], axis=1
        )
        terms = []
        for _ in range(3):
            low = rest.astype(bf16)
            terms.append(low)
            rest = rest - low.astype(f32)
        stack = jnp.concatenate([t.astype(f32) for t in terms], axis=0).astype(bf16)

        def one(i, carry):
            for u in range(4):
                at = i * 4 + u
                got = jnp.dot(stack, spread_of(at), preferred_element_type=f32)
                got = got[:heads] + got[heads : 2 * heads] + got[2 * heads :]
                for v in range(2):
                    piece = got[:, v * span : (v + 1) * span]
                    m = 2 * at + v
                    bias_t[m, : heads // 2, :span] = piece[: heads // 2]
                    bias_t[m, : heads // 2, span:] = piece[heads // 2 :]
            return carry

        lax.fori_loop(start, stop, one, 0)
        for pair in range(heads // 2 if final else 0):
            bias_s[pair] = bias_t[:, pair, :]

    def table_step(i, carry):
        for u in range(4):
            at = i * 4 + u
            one, two = dtab_s[:, at * 2, :], dtab_s[:, at * 2 + 1, :]
            part = jnp.concatenate(
                [
                    jnp.concatenate([one[:, :span], two[:, :span]], axis=1),
                    jnp.concatenate([one[:, span:], two[:, span:]], axis=1),
                ],
                axis=0,
            )
            high = part.astype(bf16).astype(f32)
            both = jnp.concatenate([high, part - high], axis=0).astype(bf16)
            carry = carry + lax.dot_general(
                both, spread_of(at), contract_last, preferred_element_type=f32
            )
        return carry

    pending = []

    def swap(index, source, target, device):
        copy = remote(source, target, red_send.at[index], red_recv.at[index], device)
        copy.start()
        pending.append(copy)
        return copy

    away, over = (x + 1) % 2, (dp + 1) % 2

    def grad_block(g):
        at = pl.ds(pl.multiple_of(g * out_width, out_width), out_width)
        block = lax.dot_general(
            att_s[...], cot_s[:, at], contract_first, preferred_element_type=f32
        )
        gb[g] = block.astype(bf16).reshape(gb.shape[1:])

    def grad_make():
        sent = []
        for i, d in enumerate((over, dp)):
            grad_block(core * 2 + d)
            sent.append(swap(8 + i, gb.at[core * 2 + d], core_g.at[d], over_core))
        for d in (over, dp):
            grad_block(col * 2 + d)
        return sent

    half_rows = st.shape[4]

    def grad_first(got):
        sent = []
        for i, d in enumerate((over, dp)):
            got[i].wait_recv()
            for r in range(rows):
                total = (gb[col * 2 + d, r].astype(f32) + core_g[d, r].astype(f32)).astype(bf16)
                st[0, d, r % 2, r // 2] = total[:half_rows]
                st[1, d, r % 2, r // 2] = total[half_rows:]
            if i == 0:
                sent.append(swap(1, st.at[0, over], a1, over_y))
        sent.append(swap(2, st.at[1, :, away], b1, over_x))
        return sent

    def grad_second(got):
        got[0].wait_recv()
        t2a[...] = (st[0, dp, away].astype(f32) + a1[away].astype(f32)).astype(bf16)
        sent = [swap(3, t2a, a2, over_x)]
        got[1].wait_recv()
        t2b[...] = (st[1, over, x].astype(f32) + b1[over].astype(f32)).astype(bf16)
        sent.append(swap(4, t2b, b2, over_y))
        keep[0] = st[0, dp, x].astype(f32) + a1[x].astype(f32)
        keep[1] = st[1, dp, x].astype(f32) + b1[dp].astype(f32)
        return sent

    def grad_third(got):
        sent = []
        for h, ref in enumerate((a2, b2)):
            got[h].wait_recv()
            keep[h] += ref[...].astype(f32)
            for s in range(1, ring):
                zs[s, h] = keep[h, (z + s) % ring].astype(bf16)
                sent.append(
                    swap(
                        10 + s * 2 + h, zs.at[s, h], zr.at[s, h],
                        {"row": ((z + s) % ring) * 2 + x},
                    )
                )
        return sent

    def grad_last(got):
        for copy in got:
            copy.wait_recv()
        for h in range(2):
            total = keep[h, z]
            for s in range(1, ring):
                total = total + zr[s, h].astype(f32)
            grad_out[h * half_rows : (h + 1) * half_rows] = total

    def unrolled(body):
        def several(i, carry):
            for u in range(UNROLL):
                body(i * UNROLL + u, carry)
            return carry

        lax.fori_loop(0, heads // 2 // UNROLL, several, 0)

    local[0].wait()
    local[1].wait()
    every = parts + 1

    def hops(h):
        for a in range(every):
            hop(a, h)

    hops(0)
    patchify()
    for copy in pat_halos:
        copy.start()
    local[2].wait()
    cot_side.start()
    cot_down[0].start()
    hops(1)
    bias_make(0, cells // 16, False)
    for copy in cot_down[1:]:
        copy.start()
    hops(2)
    for copy in pat_halos:
        copy.wait_recv()
    lax.fori_loop(0, windows // 2, prologue, 0)
    hops(3)
    lax.fori_loop(windows // 2, windows, prologue, 0)
    hops(4)
    bias_make(cells // 16, cells // 8, True)
    for copy in cot_down:
        copy.wait_recv()
    cot_corner.start()
    hops(5)
    cot_side.wait_recv()
    cot_corner.wait_recv()
    lax.fori_loop(0, windows, pick_cot, 0)
    for a in range(parts):
        partner(a)
    project()
    unrolled(attend)
    got = grad_make()
    partner(last_a)
    attended_cot()
    got = grad_first(got)
    unrolled(attend_back)
    tab = lax.fori_loop(0, cells // 8, table_step, jnp.zeros((2 * heads, 256), f32))
    tab = tab[:heads] + tab[heads:]
    got = grad_second(got)
    back_project()
    got = grad_third(got)
    gain_sum = lax.fori_loop(0, windows, finish, jnp.zeros((1, features), f32))
    patch = pat_s[...]
    embed = lax.dot_general(patch, cot_s[...], contract_first, preferred_element_type=f32)
    embed = embed + lax.dot_general(patch, norm_s[...], contract_first, preferred_element_type=f32)
    depth = embed.shape[0]
    wide = features // cols
    for c in range(cols):
        for rg in range(depth // 8):
            for lh in range(wide // 256):
                at = c * wide + lh * 256
                small_s[c, rg * (wide // 256) + lh] = embed[rg * 8 : rg * 8 + 8, at : at + 256]
    per = wide // 256
    base = patch_width // 8
    for c in range(cols):
        for lh in range(per):
            at = c * wide + lh * 256
            small_s[c, base * per + lh, 1:2] = gain_sum[:, at : at + 256]
    small_s[0, base * per, 2:8] = tab[: heads // 2]
    small_s[0, (base + 1) * per, 0 : heads // 2] = tab[heads // 2 :]
    flip = remote(small_s.at[core], core_e, sml_send.at[0], sml_recv.at[0], over_core)
    flip.start()
    flip.wait_recv()
    es[...] = (small_s[col] + core_e[...]).astype(bf16)
    spread = []
    for r in range(rows):
        for d in range(dps):
            if r or d:
                to_row, to_dp = (row + r) % rows, (dp + d) % dps
                index = r * dps + d
                copy = remote(
                    es.at[to_row * dps + to_dp], er.at[index], sml_send.at[index], sml_recv.at[index],
                    {"row": to_row, "dp": to_dp},
                )
                copy.start()
                spread.append(copy)
    mine = row * dps + dp
    for copy in spread:
        copy.wait_recv()
    whole = small_s[col, mine] + core_e[mine]
    for index in range(1, rows * dps):
        whole = whole + er[index].astype(f32)
    fin[col, mine] = whole.astype(bf16)
    tell = []
    hand = remote(fin.at[col, mine], fin.at[col, mine], fwd_send.at[0], fwd_recv.at[0], over_core)
    for r in range(rows):
        for d in range(dps):
            if r or d:
                index = r * dps + d
                copy = remote(
                    fin.at[col, mine], fin.at[col, mine], all_send.at[index], all_recv.at[index],
                    {"row": (row + r) % rows, "dp": (dp + d) % dps},
                )
                copy.start()
                tell.append(copy)
    hand.start()
    grad_last(got)
    for r in range(rows):
        for d in range(dps):
            if r or d:
                index = r * dps + d
                part = ((row + rows - r) % rows) * dps + (dp + dps - d) % dps
                place = fin.at[col, part]
                remote(place, place, all_send.at[index], all_recv.at[index], over_core).wait_recv()
                copy = remote(place, place, fwd_send.at[index], fwd_recv.at[index], over_core)
                copy.start()
                tell.append(copy)
    for r in range(rows):
        for d in range(dps):
            index = r * dps + d
            part = ((row + rows - r) % rows) * dps + (dp + dps - d) % dps
            place = fin.at[core, part]
            remote(place, place, fwd_send.at[index], fwd_recv.at[index], over_core).wait_recv()
    for c in range(cols):
        for lh in range(per):
            at = c * wide + lh * 256
            for rg in range(base):
                embed_out[rg * 8 : rg * 8 + 8, at : at + 256] = fin[c, rg * per + lh].astype(f32)
            rest = fin[c, base * per + lh].astype(f32)
            bias_out[:, at : at + 256] = rest[0:1]
            gain_out[:, at : at + 256] = rest[1:2]
    entries_out = table_out.shape[1]
    ones = fin[0, base * per].astype(f32)[:, :entries_out]
    twos = fin[0, (base + 1) * per].astype(f32)[:, :entries_out]
    for i in range(heads // 2):
        table_out[2 * i : 2 * i + 1] = ones[2 + i : 3 + i]
        table_out[2 * i + 1 : 2 * i + 2] = twos[i : i + 1]
    for copy, when in started:
        pl.when(when)(copy.wait_send)
    for copy in halos + pending + [flip] + spread + tell + [hand]:
        copy.wait_send()


def direct_device(
    sizes, pixels, cotangent, embed_weight, embed_bias, layer_norm_gain,
    qkv_weight, out_weight, bias_table, rel_index, shifts,
):
    rows, cols, dps = sizes
    ring = rows // 2
    heads, table_size = bias_table.shape
    patch_width, features = embed_weight.shape
    bf16, f32 = jnp.bfloat16, jnp.float32
    _, rows_dev, cols_dev, _ = cotangent.shape
    groups = cols * dps
    depth = 64
    cells = WIN * WIN
    inner = out_weight.shape[0] * rows
    here = rows_dev * cols_dev
    big = out_weight.shape
    half = big[0] // 2
    dma = pltpu.SemaphoreType.DMA
    vmem = pl.BlockSpec(memory_space=VMEM)
    sums = (rows * dps, 8, 256)
    grad, embed, bias, gain, table = pl.pallas_call(
        functools.partial(whole_kernel, sizes, heads, patch_width),
        out_shape=[
            jax.ShapeDtypeStruct(big, f32),
            jax.ShapeDtypeStruct((patch_width, features), f32),
            jax.ShapeDtypeStruct((1, features), f32),
            jax.ShapeDtypeStruct((1, features), f32),
            jax.ShapeDtypeStruct((heads, table_size), f32),
        ],
        in_specs=[pl.BlockSpec(memory_space=pltpu.SMEM)] + [pl.BlockSpec(memory_space=pl.ANY)] * 3 + [vmem] * 6,
        out_specs=[vmem] * 5,
        scratch_shapes=[
            VMEM((groups, rows) + qkv_weight.shape[::-1], bf16),
            VMEM((groups, rows) + big, bf16),
            VMEM((rows_dev, cols_dev, features), bf16),
            VMEM((rows_dev, cols_dev, depth), bf16),
            VMEM((cells, 2 * cells), jnp.int32),
            VMEM((cells, 8 * pl.cdiv(heads, 16), 4 * cells), f32),
            VMEM((heads // 2, cols_dev // (2 * WIN), 2 * cells, 4 * cells), f32),
            VMEM((rows_dev, WIN, features), bf16),
            VMEM((rows_dev - 1, cols_dev, features), bf16),
            VMEM((rows_dev - 1, WIN, features), bf16),
            VMEM((rows_dev, WIN, depth), bf16),
            VMEM((rows_dev - 1, cols_dev, depth), bf16),
            VMEM((rows_dev - 1, WIN, depth), bf16),
            VMEM((here, depth), bf16),
            VMEM((here, features), bf16),
            VMEM((here, features), f32),
            VMEM((here, 128), f32),
            VMEM((here, features), bf16),
            VMEM((here, 3 * inner), bf16),
            VMEM((here, inner), bf16),
            VMEM((here, inner), bf16),
            VMEM((here, 3 * inner), bf16),
            VMEM((heads // 2, cells, 4 * cells), f32),
            VMEM((heads // 2, cells, 4 * cells), f32),
            VMEM((here, features), f32),
            VMEM((groups, rows) + big, bf16),
            VMEM((2, rows) + big, bf16),
            VMEM((2, 2, 2, ring, half, big[1]), bf16),
            VMEM((2, ring, half, big[1]), bf16),
            VMEM((2, ring, half, big[1]), bf16),
            VMEM((ring, half, big[1]), bf16),
            VMEM((ring, half, big[1]), bf16),
            VMEM((ring, half, big[1]), bf16),
            VMEM((ring, half, big[1]), bf16),
            VMEM((2, ring, half, big[1]), f32),
            VMEM((ring, 2, half, big[1]), bf16),
            VMEM((ring, 2, half, big[1]), bf16),
            VMEM((cols,) + sums, f32),
            VMEM(sums, f32), VMEM(sums, bf16), VMEM(sums, bf16),
            VMEM((cols,) + sums, bf16),
            dma((400,)), dma((3, 8 * ring)), dma((3,)), dma((16,)), dma((16,)),
            dma((20,)), dma((20,)),
            dma((rows * dps,)), dma((rows * dps,)), dma((rows * dps,)), dma((rows * dps,)),
            dma((rows * dps,)), dma((rows * dps,)),
        ],
        compiler_params=pltpu.CompilerParams(
            collective_id=0, has_side_effects=True, vmem_limit_bytes=60 * 2**20
        ),
        name="whole",
    )(
        shifts, qkv_weight.T, out_weight, cotangent, pixels, embed_weight,
        embed_bias[None], layer_norm_gain[None], bias_table, rel_index,
    )
    results = (grad, embed, bias, gain, table)
    grad, embed, bias, gain, table = pl.pallas_call(
        hand_out,
        out_shape=[jax.ShapeDtypeStruct(value.shape, value.dtype) for value in results],
        in_specs=[vmem] * 5,
        out_specs=[pl.BlockSpec(memory_space=pl.ANY)] * 5,
        scratch_shapes=[dma((5,))],
        name="hand_out",
    )(*results)
    return (grad, embed, bias[0], gain[0], table)


def solution(mesh):
    sizes = tuple(mesh.shape[name] for name in ("row", "col", "dp"))
    direct = sizes[1:] == (2, 2) and sizes[0] == 8
    return jax.shard_map(
        functools.partial(direct_device if direct else on_device, sizes),
        mesh=mesh,
        in_specs=(
            P("dp", None, "row", "col"),
            P("dp", "row", "col", None),
            P(),
            P(),
            P(),
            P("row", ("col", "dp")),
            P("row", ("col", "dp")),
            P(),
            P(),
            P("dp", None),
        ),
        out_specs=(P("row", ("col", "dp")), P(), P(), P(), P()),
        check_vma=False,
    )
```
